256 devices in a mesh: seq: 16 (over z, core), tp: 8 (over x_lo, y), dp: 2 (over x_hi).
Axes of the slice: x: 4 (x_hi: 2, x_lo: 2; x = x_hi * 2 + x_lo), y: 4, z: 8, core: 2. Of those that a mesh axis runs over, the one named last changes fastest.
Arguments:
- query_latent: bfloat16 [2, 4096, 1536], P('dp', 'seq', 'tp'), may hold values from -6 to 6
- key_latent: bfloat16 [2, 4096, 512], P('dp', 'seq', 'tp'), may hold values from -6 to 6
- rope_key: bfloat16 [2, 4096, 64], P('dp', 'seq'), may hold values from -6 to 6
- w_uq: bfloat16 [1536, 12288], P('seq', 'tp')
- w_uk: bfloat16 [512, 8192], P('seq', 'tp'), may hold values from -0.25 to 0.25
- w_uv: bfloat16 [512, 8192], P('seq', 'tp'), may hold values from -0.25 to 0.25
- block_order: int32 [2, 32], P('dp'), may hold values from 0 to 31, each once within a row
- segment_ids: int32 [2, 4096], P('dp'), may hold values from 0 to 3, never falling along the last dimension, each value on 1 to 2048 neighbouring positions
Outputs:
- context: bfloat16 [2, 4096, 8192], P('dp', 'seq', 'tp')
- clipped_uq: bfloat16 [1536, 12288], P('seq', 'tp')
- clipped_uk: bfloat16 [512, 8192], P('seq', 'tp')
The draws below stay inside these ranges and needn't reach their ends.
Inputs may be any that keep to these rules, and one draw needn't show every extreme that they name: `block_order`: each row is a permutation of the 32 position blocks. `segment_ids`: never falling along positions; each document has at most 2048 positions.
All inputs are finite; a program needn't handle non-finite values.
Results may differ from the reference program's by a relative error of at most 0.012.
The reference program's roundings to bfloat16 on the way (of `weights`) count: a program that leaves them out, or rounds other values in their place, can miss the bound.
Values may be sent and summed in bfloat16 or wider, within the bound.
No kernel may reach another device: no remote copies, remote signals or barrier semaphores. Data moves between devices by JAX's collectives and lax.ppermute only.
A program may use at most 64 MiB of HBM per device.

```python
import math
import jax
import jax.numpy as jnp
import numpy as np
from jax import lax

HEADS = 64
NOPE = 128
ROPE = 64
VD = 128
QL = 1536
KL = 512
TOK_DEV = 256
CLIP = 8
L = 4096
BLOCKS = 32
SEQS = 2
N_DP = 2


def draw_w_uq(key, part):
    first, second = jax.random.split(jax.random.fold_in(key, 11))
    base = jax.random.normal(first, (QL, HEADS * (NOPE + ROPE)), jnp.float32) * QL ** (-0.5)
    lowest, highest = (math.log(0.5), math.log(3.0))
    exponent = jax.random.uniform(second, (HEADS,), jnp.float32, lowest, highest)
    factor = jnp.repeat(jnp.exp(exponent), NOPE + ROPE)
    return (base * factor[None, :]).astype(jnp.bfloat16)


def shard_levels(stream_key, shape, pieces, least, top_value):
    def one(axis_at, blocks):
        draws = jax.random.uniform(jax.random.fold_in(jax.random.fold_in(stream_key, 6), axis_at), (blocks,), jnp.float32, least / len(pieces), top_value / len(pieces))
        return jnp.repeat(jnp.exp(draws), shape[axis_at] // blocks).reshape((-1,) + (1,) * (len(shape) - axis_at - 1))

    level = one(*pieces[0])
    for cut in pieces[1:]:
        level = level * one(*cut)
    return level


def length_profile(amount, total, reach, slope):
    portions = [(1 << 20) // math.isqrt(rank ** slope) + 1 for rank in range(2, amount + 1)]
    rest, counts = total - reach - (amount - 1), [1] * (amount - 1)
    while rest > 0:
        free = [i for i in range(amount - 1) if counts[i] < reach]
        pool, remaining = sum([portions[i] for i in free]), rest
        for i in free:
            extra = min(reach - counts[i], max(1, remaining * portions[i] // pool), rest)
            counts[i] = counts[i] + extra
            rest = rest - extra
    return np.array([reach] + counts)


def ragged(own_key, number_of, total, limit, slope):
    if number_of == 2:
        one = jax.random.randint(own_key, (), max(1, total - limit), min(limit, total - 1) + 1)
        return jnp.stack([one, total - one])
    lengths = jnp.asarray(length_profile(number_of, total, limit, slope), jnp.int32)
    twos = (number_of - 1) // 2
    giver, taker = lengths[1:1 + 2 * twos:2], lengths[2:2 + 2 * twos:2]
    room = jnp.minimum(giver - 1, limit - taker)
    moved = jax.random.randint(jax.random.fold_in(own_key, 1), (twos,), 0, 1 << 20) % (room + 1)
    lengths = lengths.at[1:1 + 2 * twos:2].set(giver - moved).at[2:2 + 2 * twos:2].set(taker + moved)
    return lengths[jax.random.permutation(jax.random.fold_in(own_key, 2), number_of)]


def centred(rng, extent, deviation, bound, cuts=(), kind=jnp.bfloat16):
    level = shard_levels(rng, extent, cuts, -0.22, 0.18) if cuts else 1.0
    drawn = jax.random.normal(rng, extent, jnp.float32) * deviation * level
    return jnp.minimum(jnp.maximum(drawn, -bound), bound).astype(kind)


def setup_inputs(seed: int = 0) -> dict:
    splits = jax.random.split(jax.random.key(seed), 9)
    query_latent = centred(splits[0], (SEQS, L, QL), 1.0, 6.0, ((0, 2), (1, 16), (2, 8)))
    key_latent = centred(splits[1], (SEQS, L, KL), 1.0, 6.0, ((0, 2), (1, 16), (2, 8)))
    rope_key = centred(splits[2], (SEQS, L, ROPE), 1.0, 6.0, ((0, 2), (1, 16)))
    w_uq = draw_w_uq(jax.random.fold_in(splits[8], 71), 0)
    w_uk = centred(splits[4], (KL, HEADS * NOPE), KL ** -0.5, 0.25, ((0, 16), (1, 8)))
    w_uv = centred(splits[5], (KL, HEADS * VD), KL ** -0.5, 0.25, ((0, 16), (1, 8)))
    block_order = jax.vmap(lambda own: jax.random.permutation(own, BLOCKS))(jax.random.split(splits[6], SEQS)).reshape((SEQS, BLOCKS)).astype(jnp.int32)
    segment_ids = jax.vmap(lambda own: jnp.searchsorted(jnp.cumsum(ragged(own, 4, L, L // 2, 1)), jnp.arange(L), side="right"))(jax.random.split(splits[7], SEQS)).reshape((SEQS, L)).astype(jnp.int32)
    return {"query_latent": query_latent, "key_latent": key_latent, "rope_key": rope_key, "w_uq": w_uq, "w_uk": w_uk, "w_uv": w_uv, "block_order": block_order, "segment_ids": segment_ids}


rope_base = 50000.0
masked_value = -1e+30

def turning(positions, width):
    steps = jnp.arange(width // 2, dtype=jnp.float32) * (2.0 / width)
    freqs = jnp.exp(-math.log(rope_base) * steps)
    angle = positions.astype(jnp.float32)[:, None] * freqs[None, :]
    return (jnp.cos(angle), jnp.sin(angle))

def rotate(values, cosine, sine):
    half = values.shape[-1] // 2
    first = values[..., :half]
    second = values[..., half:]
    return jnp.concatenate([first * cosine - second * sine, second * cosine + first * sine], axis=-1)

def stored_positions(order, half_block):
    count = order.shape[0] * half_block
    index = jnp.arange(count, dtype=jnp.int32)
    return (jnp.take(order, index // half_block) * half_block + index % half_block).astype(jnp.int32)

def reference(query_latent, key_latent, rope_key, w_uq, w_uk, w_uv, block_order, segment_ids):
    half_block = TOK_DEV // 2
    scale = 1.0 / math.sqrt(NOPE + ROPE)
    contexts = []
    largest = jnp.full((HEADS,), masked_value, jnp.float32)
    for member in range(N_DP):
        positions = stored_positions(block_order[member], half_block)
        labels = jnp.take(segment_ids[member], positions)
        cosine, sine = turning(positions, ROPE)
        query_full = jnp.dot(query_latent[member], w_uq, preferred_element_type=jnp.float32).reshape(L, HEADS, NOPE + ROPE)
        query_nope = query_full[:, :, :NOPE].astype(jnp.bfloat16)
        query_rope = rotate(query_full[:, :, NOPE:], cosine[:, None, :], sine[:, None, :]).astype(jnp.bfloat16)
        key_nope = jnp.dot(key_latent[member], w_uk, preferred_element_type=jnp.float32).astype(jnp.bfloat16).reshape(L, HEADS, NOPE)
        values = jnp.dot(key_latent[member], w_uv, preferred_element_type=jnp.float32).astype(jnp.bfloat16).reshape(L, HEADS, VD)
        key_rope = rotate(rope_key[member].astype(jnp.float32), cosine, sine).astype(jnp.bfloat16)
        allowed = (positions[None, :] <= positions[:, None]) & (labels[None, :] == labels[:, None])

        def one_head(inputs):
            head_qn, head_qr, head_kn, head_values = inputs
            scores = jnp.dot(head_qn, head_kn.T, preferred_element_type=jnp.float32)
            scores = (scores + jnp.dot(head_qr, key_rope.T, preferred_element_type=jnp.float32)) * scale
            masked = jnp.where(allowed, scores, masked_value)
            row_max = lax.optimization_barrier(jnp.max(masked, axis=1))
            weights = jnp.where(allowed, jnp.exp(masked - row_max[:, None]), 0.0)
            total = lax.optimization_barrier(jnp.sum(weights, axis=1))
            mixed = jnp.dot(weights.astype(jnp.bfloat16), head_values, preferred_element_type=jnp.float32)
            return ((mixed / total[:, None]).astype(jnp.bfloat16), jnp.max(row_max))
        per_head, head_max = lax.map(one_head, (jnp.transpose(query_nope, (1, 0, 2)), jnp.transpose(query_rope, (1, 0, 2)), jnp.transpose(key_nope, (1, 0, 2)), jnp.transpose(values, (1, 0, 2))))
        contexts.append(jnp.transpose(per_head, (1, 0, 2)).reshape(L, HEADS * VD))
        largest = jnp.maximum(largest, head_max)
    ratio = CLIP / jnp.maximum(largest, CLIP)
    root = jnp.sqrt(ratio)
    factors = jnp.concatenate([jnp.broadcast_to(root[:, None], (HEADS, NOPE)), jnp.broadcast_to(ratio[:, None], (HEADS, ROPE))], axis=1).reshape(HEADS * (NOPE + ROPE))
    clipped_uq = (w_uq.astype(jnp.float32) * factors[None, :]).astype(jnp.bfloat16)
    clipped_uk = (w_uk.astype(jnp.float32) * jnp.repeat(root, NOPE)[None, :]).astype(jnp.bfloat16)
    return (jnp.stack(contexts), clipped_uq, clipped_uk)
```

```python
import math

import jax
import jax.numpy as jnp
from jax import lax
from jax.experimental import pallas as pl
from jax.experimental.pallas import tpu as pltpu
from jax.sharding import PartitionSpec as P

NOPE = 128
ROPE = 64
VD = 128
CLIP = 8
BLK = 128
CHUNK = 256

rope_base = 50000.0
masked_value = -1e30
scale = 1.0 / math.sqrt(NOPE + ROPE)

ANY = pl.BlockSpec(memory_space=pl.ANY)
SMEM = pl.BlockSpec(memory_space=pltpu.SMEM)
VMEM = pl.BlockSpec(memory_space=pltpu.VMEM)


def meta_of(meta):
    return dict(z=meta[35], c=meta[36], y=meta[37], xl=meta[38])


def block_of(meta, i):
    m = meta_of(meta)
    half = i // 2
    core = jnp.where(half == 0, m["c"], 1 - m["c"])
    return meta[(m["z"] * 2 + core) * 2 + i % 2]


def start_of(meta, p):
    s = jnp.int32(0)
    for l in range(3):
        b = meta[32 + l]
        s = jnp.where(b <= p, jnp.maximum(s, b), s)
    return s


def chunk_range(meta, i):
    pb = block_of(meta, i)
    lo = start_of(meta, pb * BLK) // CHUNK
    return pb, lo, (pb * BLK) // CHUNK + 1


def feature_row(meta, t, each):
    m = meta_of(meta)
    x, yy = t // 4, t % 4
    dy = lax.rem(yy - m["y"] + 4, 4)
    j = jnp.where(dy == 0, 0, jnp.where(dy == 1, 2, jnp.where(dy == 2, 3, 1)))
    xr = jnp.where(x == m["xl"], 0, 1)
    return (j * 2 + xr) * each


RING = [0, -1, 1, -2, 2, -3, 3, -4]


def project_kernel(meta, *refs):
    lat_in, kv_in = refs[:16], refs[16:24]
    kn_out, v_out, kr_out = refs[24:27]
    lat, kvw, sem, wsem = refs[27:]
    m = meta_of(meta)
    wcopies = []
    for j in range(8):
        t = lax.rem(m["z"] + RING[j] + 8, 8)
        row = pl.multiple_of(feature_row(meta, t, 64), 64)
        cp = pltpu.make_async_copy(kv_in[j], kvw.at[pl.ds(row, 64)], wsem.at[j])
        cp.start()
        wcopies.append(cp)
    copies = []
    for i in range(16):
        cp = pltpu.make_async_copy(lat_in[i], lat.at[i], sem.at[i])
        cp.start()
        copies.append(cp)
    for cp in wcopies:
        cp.wait()
    for cp in copies:
        cp.wait()

    def step(i, carry):
        j = lax.rem(i, 8)
        s = (j + 1) // 2
        dz = jnp.where(lax.rem(j, 2) == 1, -s, s)
        zz = lax.rem(m["z"] + dz + 8, 8)
        cc = jnp.where(i < 8, m["c"], 1 - m["c"])
        base = (zz * 2 + cc) * 2
        out = jnp.dot(lat[i, :, : 4 * 128], kvw[...], preferred_element_type=jnp.float32)
        for b in range(2):
            pb = pl.multiple_of(meta[base + b] * BLK, BLK)
            rows = slice(b * BLK, (b + 1) * BLK)
            kn_out[pl.ds(pb, BLK), :] = out[rows, :512].astype(jnp.bfloat16)
            v_out[pl.ds(pb, BLK), :] = out[rows, 512:].astype(jnp.bfloat16)
            kr_out[pl.ds(pb, BLK), :] = lat[i, rows, 512:]
        return carry

    lax.fori_loop(0, 16, step, 0)


def bias_of(meta, pb, ch):
    row = lax.broadcasted_iota(jnp.int32, (BLK, CHUNK), 0) + pb * BLK
    col = lax.broadcasted_iota(jnp.int32, (BLK, CHUNK), 1) + ch * CHUNK
    start = jnp.zeros_like(row)
    for l in range(3):
        b = meta[32 + l]
        start = jnp.where(row >= b, jnp.maximum(start, b), start)
    allowed = (col <= row) & (col >= start)
    return jnp.where(allowed, 0.0, masked_value)


def scores_of(qs_h, kn, kr, ch, h):
    rows = pl.ds(pl.multiple_of(ch * CHUNK, CHUNK), CHUNK)
    k = jnp.concatenate([kn[rows, h * 128 : (h + 1) * 128], kr[rows, :]], axis=1)
    return lax.dot_general(qs_h, k, (((1,), (1,)), ((), ())), preferred_element_type=jnp.float32)


def max_kernel(meta, qown, qsib, w_in, cs, kn, kr, qs_out, rm_out, hm_out, w, sem, mx):
    m = meta_of(meta)
    copies = []
    for t in range(8):
        row = pl.multiple_of(feature_row(meta, t, 192), 64)
        cp = pltpu.make_async_copy(w_in.at[pl.ds(t * 192, 192)], w.at[pl.ds(row, 192)], sem.at[t])
        cp.start()
        copies.append(cp)
    for cp in copies:
        cp.wait()
    for half, q_in in enumerate((qown, qsib)):
        q = jnp.dot(q_in[...], w[...], preferred_element_type=jnp.float32)
        rows = slice(half * 256, half * 256 + 256)
        cos = cs[rows, :64]
        sin = cs[rows, 64:]
        for h in range(4):
            nope = q[:, h * 192 : h * 192 + 128].astype(jnp.bfloat16)
            r = q[:, h * 192 + 128 : h * 192 + 192]
            turned = jnp.concatenate([r[:, 32:], r[:, :32]], axis=1)
            rot = (r * cos + turned * sin).astype(jnp.bfloat16)
            qs_out[h, rows, :128] = nope
            qs_out[h, rows, 128:] = jnp.concatenate([rot, jnp.zeros_like(rot)], axis=1)

    hm_out[...] = jnp.full(hm_out.shape, masked_value, jnp.float32)

    def q_block(i, carry):
        pb, lo, hi = chunk_range(meta, i)
        rows = pl.ds(pl.multiple_of(i * BLK, BLK), BLK)
        mx[...] = jnp.full(mx.shape, masked_value, jnp.float32)

        def chunk(ch, carry):
            bias = bias_of(meta, pb, ch)
            for h in range(4):
                s = scores_of(qs_out[h, rows, :], kn, kr, ch, h) + bias
                mx[h] = jnp.maximum(mx[h], jnp.maximum(s[:, :128], s[:, 128:]))
            return carry

        lax.fori_loop(lo, hi, chunk, 0)
        for h in range(4):
            top = jnp.max(mx[h], axis=1, keepdims=True)
            top = jnp.broadcast_to(top, (BLK, 128))
            rm_out[h, rows, :] = top
            best = jnp.max(top, axis=0, keepdims=True) * scale
            hm_out[h : h + 1, :] = jnp.maximum(hm_out[h : h + 1, :], best)
        return carry

    lax.fori_loop(0, 4, q_block, 0)


def mix_kernel(meta, qs, rm, kn, kr, v, out, acc, total):
    def q_block(i, carry):
        pb, lo, hi = chunk_range(meta, i)
        rows = pl.ds(pl.multiple_of(i * BLK, BLK), BLK)
        acc[...] = jnp.zeros(acc.shape, jnp.float32)
        total[...] = jnp.zeros(total.shape, jnp.float32)

        def chunk(ch, carry):
            bias = bias_of(meta, pb, ch)
            keys = pl.ds(pl.multiple_of(ch * CHUNK, CHUNK), CHUNK)
            for h in range(4):
                s = scores_of(qs[h, rows, :], kn, kr, ch, h) + bias
                top = rm[h, rows, :]
                p0 = jnp.exp2((s[:, :128] - top) * (scale * math.log2(math.e)))
                p1 = jnp.exp2((s[:, 128:] - top) * (scale * math.log2(math.e)))
                total[h] += p0 + p1
                p = jnp.concatenate([p0, p1], axis=1).astype(jnp.bfloat16)
                acc[h] += jnp.dot(
                    p, v[keys, h * 128 : (h + 1) * 128], preferred_element_type=jnp.float32
                )
            return carry

        lax.fori_loop(lo, hi, chunk, 0)
        for h in range(4):
            whole = jnp.sum(total[h], axis=1, keepdims=True)
            out[rows, h * 128 : (h + 1) * 128] = (acc[h] / whole).astype(jnp.bfloat16)
        return carry

    lax.fori_loop(0, 4, q_block, 0)


def shift_seq(by):
    return [(i, (i + 2 * by) % 16) for i in range(16)]


SWAP = [(i, i ^ 1) for i in range(16)]
XSWAP = [(i, i ^ 4) for i in range(8)]


def shift_y(by):
    return [(x * 4 + y, x * 4 + (y + by) % 4) for x in range(2) for y in range(4)]


def ring(x):
    up, dn, got = x, x, [x]
    for s in range(4):
        up = lax.ppermute(up, "seq", shift_seq(1))
        got.append(up)
        if s < 3:
            dn = lax.ppermute(dn, "seq", shift_seq(-1))
            got.append(dn)
    return got


def swap(x):
    return lax.ppermute(x, "seq", SWAP)


def halves(w, c, width):
    mine = lax.dynamic_slice_in_dim(w, c * width, width, 1)
    other = swap(lax.dynamic_slice_in_dim(w, (1 - c) * width, width, 1))
    first = c == 0
    return jnp.concatenate([jnp.where(first, mine, other), jnp.where(first, other, mine)], axis=0)


def of_everyone(array, axis):
    copies = jnp.broadcast_to(array, (lax.axis_size(axis), *array.shape))
    return jnp.max(lax.all_to_all(copies, axis, split_axis=0, concat_axis=0, tiled=True), axis=0)


def on_device(query_latent, key_latent, rope_key, w_uq, w_uk, w_uv, block_order, segment_ids):
    bf16, f32 = jnp.bfloat16, jnp.float32
    s, t = lax.axis_index("seq"), lax.axis_index("tp")
    z, c, y, xl = s // 2, s % 2, t % 4, t // 4
    order, labels = block_order[0], segment_ids[0]
    bounds = jnp.stack([jnp.sum((labels < l).astype(jnp.int32)) for l in (1, 2, 3)])
    meta = jnp.concatenate(
        [order, bounds, jnp.stack([z, c, y, xl]).astype(jnp.int32), jnp.zeros((9,), jnp.int32)]
    )

    wq = halves(w_uq, c, 768)
    kv = halves(
        jnp.concatenate([w_uk[:, :512], w_uv[:, :512], w_uk[:, 512:], w_uv[:, 512:]], axis=1), c, 1024
    )
    groups = [[2 * i for i in range(8)], [2 * i + 1 for i in range(8)]]
    w_all = lax.all_gather(wq, "seq", axis=0, tiled=True, axis_index_groups=groups)

    chip = lax.dynamic_slice_in_dim(order, 4 * z, 4)
    chip = jnp.where(c == 0, chip, jnp.roll(chip, 2))
    pos = (chip[:, None] * BLK + jnp.arange(BLK, dtype=jnp.int32)[None, :]).reshape(-1)
    steps = jnp.arange(ROPE // 2, dtype=f32) * (2.0 / ROPE)
    freqs = jnp.exp(-math.log(rope_base) * steps)
    angle = pos.astype(f32)[:, None] * freqs[None, :]
    cos, sin = jnp.cos(angle), jnp.sin(angle)
    cs = jnp.concatenate([cos, cos, -sin, sin], axis=1)

    kq = jnp.concatenate([key_latent[0].T, query_latent[0].T], axis=0)
    kq_x = lax.ppermute(kq, "tp", XSWAP)
    kq = jnp.concatenate([kq[:64], kq_x[:64], kq[64:], kq_x[64:]], axis=0).T
    parts = [kq] + [lax.ppermute(kq, "tp", shift_y(by)) for by in (1, -1, 2)]
    q_own = jnp.concatenate([p[:, 128:] for p in parts], axis=1)
    rk = rope_key[0].astype(f32)
    a, b = rk[:, :32], rk[:, 32:]
    rc, rs = cos[:256], sin[:256]
    k_rope = jnp.concatenate([a * rc - b * rs, b * rc + a * rs], axis=1).astype(bf16)
    k_own = jnp.concatenate(
        [p[:, :128] for p in parts] + [k_rope, jnp.zeros_like(k_rope)], axis=1
    )
    q_sib = swap(q_own)
    kv_ring = ring(kv)
    k_ring = ring(k_own)
    k_sib = [swap(p) for p in k_ring]

    kn, v, kr = pl.pallas_call(
        project_kernel,
        out_shape=[
            jax.ShapeDtypeStruct((4096, 512), bf16),
            jax.ShapeDtypeStruct((4096, 512), bf16),
            jax.ShapeDtypeStruct((4096, 128), bf16),
        ],
        in_specs=[SMEM] + [ANY] * 24,
        out_specs=[VMEM] * 3,
        scratch_shapes=[
            pltpu.VMEM((16, 256, 640), bf16),
            pltpu.VMEM((512, 1024), bf16),
            pltpu.SemaphoreType.DMA((16,)),
            pltpu.SemaphoreType.DMA((8,)),
        ],
        cost_estimate=pl.CostEstimate(
            flops=2 * 4096 * 512 * 1024, bytes_accessed=16 << 20, transcendentals=0
        ),
        name="project",
    )(meta, *k_ring, *k_sib, *kv_ring)

    qs, rm, hm = pl.pallas_call(
        max_kernel,
        out_shape=[
            jax.ShapeDtypeStruct((4, 512, 256), bf16),
            jax.ShapeDtypeStruct((4, 512, 128), f32),
            jax.ShapeDtypeStruct((8, 128), f32),
        ],
        in_specs=[SMEM, VMEM, VMEM, ANY, VMEM, VMEM, VMEM],
        out_specs=[VMEM] * 3,
        scratch_shapes=[
            pltpu.VMEM((1536, 768), bf16),
            pltpu.SemaphoreType.DMA((8,)),
            pltpu.VMEM((4, 128, 128), f32),
        ],
        cost_estimate=pl.CostEstimate(
            flops=2 * 512 * 1536 * 768 + 2 * 512 * 2048 * 1024, bytes_accessed=12 << 20, transcendentals=0
        ),
        name="rowmax",
    )(meta, q_own, q_sib, w_all, cs, kn, kr)

    ctx = pl.pallas_call(
        mix_kernel,
        out_shape=jax.ShapeDtypeStruct((512, 512), bf16),
        in_specs=[SMEM] + [VMEM] * 5,
        out_specs=VMEM,
        scratch_shapes=[
            pltpu.VMEM((4, 128, 128), f32),
            pltpu.VMEM((4, 128, 128), f32),
        ],
        cost_estimate=pl.CostEstimate(
            flops=2 * 512 * 2048 * 2048, bytes_accessed=12 << 20, transcendentals=4 << 20
        ),
        name="mix",
    )(meta, qs, rm, kn, kr, v)

    local_max = hm[:4, 0]
    low = jnp.full((4,), masked_value, f32)
    both = jnp.where(
        c == 0, jnp.concatenate([local_max, low]), jnp.concatenate([low, local_max])
    )
    head_max = of_everyone(both, ("seq", "dp"))
    ratio = CLIP / jnp.maximum(head_max, CLIP)
    root = jnp.sqrt(ratio)
    factors = jnp.concatenate(
        [jnp.broadcast_to(root[:, None], (8, NOPE)), jnp.broadcast_to(ratio[:, None], (8, ROPE))], axis=1
    ).reshape(8 * (NOPE + ROPE))
    clipped_uq = (w_uq.astype(f32) * factors[None, :]).astype(bf16)
    clipped_uk = (w_uk.astype(f32) * jnp.repeat(root, NOPE)[None, :]).astype(bf16)

    got = swap(ctx[256:])
    own = ctx[:256]
    first = c == 0
    context = jnp.concatenate([jnp.where(first, own, got), jnp.where(first, got, own)], axis=1)
    return (context[None], clipped_uq, clipped_uk)


def solution(mesh):
    placed = (
        P("dp", "seq", "tp"),
        P("dp", "seq", "tp"),
        P("dp", "seq", None),
        P("seq", "tp"),
        P("seq", "tp"),
        P("seq", "tp"),
        P("dp", None),
        P("dp", None),
    )
    return jax.shard_map(
        on_device,
        mesh=mesh,
        in_specs=placed,
        out_specs=(P("dp", "seq", "tp"), P("seq", "tp"), P("seq", "tp")),
        check_vma=False,
    )
```

```python
import math

import jax
import jax.numpy as jnp
from jax import lax
from jax.experimental import pallas as pl
from jax.experimental.pallas import tpu as pltpu
from jax.sharding import PartitionSpec as P

NOPE = 128
ROPE = 64
VD = 128
CLIP = 8
BLK = 128
CHUNK = 256

rope_base = 50000.0
masked_value = -1e30
scale = 1.0 / math.sqrt(NOPE + ROPE)

ANY = pl.BlockSpec(memory_space=pl.ANY)
SMEM = pl.BlockSpec(memory_space=pltpu.SMEM)
VMEM = pl.BlockSpec(memory_space=pltpu.VMEM)


def meta_of(meta):
    return dict(z=meta[35], c=meta[36], y=meta[37], xl=meta[38])


def block_of(meta, i):
    m = meta_of(meta)
    half = i // 2
    core = jnp.where(half == 0, m["c"], 1 - m["c"])
    return meta[(m["z"] * 2 + core) * 2 + i % 2]


def start_of(meta, p):
    s = jnp.int32(0)
    for l in range(3):
        b = meta[32 + l]
        s = jnp.where(b <= p, jnp.maximum(s, b), s)
    return s


def chunk_range(meta, i):
    pb = block_of(meta, i)
    lo = start_of(meta, pb * BLK) // CHUNK
    return pb, lo, (pb * BLK) // CHUNK + 1


def feature_row(meta, t, each):
    m = meta_of(meta)
    x, yy = t // 4, t % 4
    dy = lax.rem(yy - m["y"] + 4, 4)
    j = jnp.where(dy == 0, 0, jnp.where(dy == 1, 2, jnp.where(dy == 2, 3, 1)))
    xr = jnp.where(x == m["xl"], 0, 1)
    return (j * 2 + xr) * each


RING = [0, -1, 1, -2, 2, -3, 3, -4]


def join_kernel(*refs):
    for j in range(8):
        refs[8][j] = refs[j][...]


def project_kernel(meta, *refs):
    pieces, kv_in = (refs[:5], refs[5:10]), refs[10:18]
    kn_out, v_out, kr_out = refs[18:21]
    lat, rope, kvw, sem, wsem = refs[21:]
    m = meta_of(meta)
    copies = []
    for j in range(8):
        t = lax.rem(m["z"] + RING[j] + 8, 8)
        row = pl.multiple_of(feature_row(meta, t, 64), 64)
        copies.append(pltpu.make_async_copy(kv_in[j], kvw.at[pl.ds(row, 64)], wsem.at[j]))
    for core in range(2):
        own, up, dn, f1, f2 = pieces[core]
        for n, (src, q, first, count, dy) in enumerate(
            ((own, 0, 0, 8, 0), (up, 1, 0, 8, 3), (dn, 2, 0, 8, 1), (f1, 3, 0, 4, 2), (f2, 3, 4, 4, 2))
        ):
            i = core * 8 + first
            yq = lax.rem(m["y"] + dy, 4)
            copies.append(
                pltpu.make_async_copy(
                    src.at[:, :256, :],
                    lat.at[pl.ds(i, count), :, pl.ds(q * 128, 128)],
                    sem.at[core, n, 0],
                )
            )
            copies.append(
                pltpu.make_async_copy(
                    src.at[:, 256:, :],
                    rope.at[pl.ds(i, count), pl.ds(pl.multiple_of(yq * 32, 32), 32), :],
                    sem.at[core, n, 1],
                )
            )
    for cp in copies:
        cp.start()
    for cp in copies:
        cp.wait()

    def step(i, carry):
        j = lax.rem(i, 8)
        s = (j + 1) // 2
        dz = jnp.where(lax.rem(j, 2) == 1, -s, s)
        zz = lax.rem(m["z"] + dz + 8, 8)
        cc = jnp.where(i < 8, m["c"], 1 - m["c"])
        base = (zz * 2 + cc) * 2
        out = jnp.dot(lat[i], kvw[...], preferred_element_type=jnp.float32)
        fold = rope[i]
        for b in range(2):
            pb = pl.multiple_of(meta[base + b] * BLK, BLK)
            rows = slice(b * BLK, (b + 1) * BLK)
            kn_out[pl.ds(pb, BLK), :] = out[rows, :512].astype(jnp.bfloat16)
            v_out[pl.ds(pb, BLK), :] = out[rows, 512:].astype(jnp.bfloat16)
            if b == 1:
                fold = jnp.concatenate([fold[:, 64:], fold[:, :64]], axis=1)
            kr_out[pl.ds(pb, BLK), :] = fold
        return carry

    lax.fori_loop(0, 16, step, 0)


def bias_of(meta, pb, ch):
    row = lax.broadcasted_iota(jnp.int32, (BLK, CHUNK), 0) + pb * BLK
    col = lax.broadcasted_iota(jnp.int32, (BLK, CHUNK), 1) + ch * CHUNK
    start = jnp.zeros_like(row)
    for l in range(3):
        b = meta[32 + l]
        start = jnp.where(row >= b, jnp.maximum(start, b), start)
    allowed = (col <= row) & (col >= start)
    return jnp.where(allowed, 0.0, masked_value)


def scores_of(qs_h, kn, kr, ch, h):
    rows = pl.ds(pl.multiple_of(ch * CHUNK, CHUNK), CHUNK)
    k = jnp.concatenate([kn[rows, h * 128 : (h + 1) * 128], kr[rows, :]], axis=1)
    return lax.dot_general(qs_h, k, (((1,), (1,)), ((), ())), preferred_element_type=jnp.float32)


def max_kernel(meta, qown, qsib, *refs):
    w_in = refs[:8]
    cs, kn, kr, qs_out, rm_out, hm_out, w, sem, mx = refs[8:]
    m = meta_of(meta)
    copies = []
    for j in range(8):
        t = lax.rem(m["z"] + RING[j] + 8, 8)
        row = pl.multiple_of(feature_row(meta, t, 192), 64)
        cp = pltpu.make_async_copy(w_in[j], w.at[pl.ds(row, 192)], sem.at[j])
        cp.start()
        copies.append(cp)
    for cp in copies:
        cp.wait()
    for half, q_in in enumerate((qown, qsib)):
        q = jnp.dot(q_in[...], w[...], preferred_element_type=jnp.float32)
        rows = slice(half * 256, half * 256 + 256)
        cos = cs[rows, :64]
        sin = cs[rows, 64:]
        for h in range(4):
            nope = q[:, h * 192 : h * 192 + 128].astype(jnp.bfloat16)
            r = q[:, h * 192 + 128 : h * 192 + 192]
            turned = jnp.concatenate([r[:, 32:], r[:, :32]], axis=1)
            rot = (r * cos + turned * sin).astype(jnp.bfloat16)
            qs_out[h, rows, :128] = nope
            qs_out[h, rows, 128:] = jnp.concatenate([rot, jnp.zeros_like(rot)], axis=1)

    hm_out[...] = jnp.full(hm_out.shape, masked_value, jnp.float32)

    def q_block(i, carry):
        pb, lo, hi = chunk_range(meta, i)
        rows = pl.ds(pl.multiple_of(i * BLK, BLK), BLK)
        mx[...] = jnp.full(mx.shape, masked_value, jnp.float32)

        def chunk(ch, carry):
            bias = bias_of(meta, pb, ch)
            for h in range(4):
                s = scores_of(qs_out[h, rows, :], kn, kr, ch, h) + bias
                mx[h] = jnp.maximum(mx[h], jnp.maximum(s[:, :128], s[:, 128:]))
            return carry

        lax.fori_loop(lo, hi, chunk, 0)
        for h in range(4):
            top = jnp.max(mx[h], axis=1, keepdims=True)
            top = jnp.broadcast_to(top, (BLK, 128))
            rm_out[h, rows, :] = top
            best = jnp.max(top, axis=0, keepdims=True) * scale
            hm_out[h : h + 1, :] = jnp.maximum(hm_out[h : h + 1, :], best)
        return carry

    lax.fori_loop(0, 4, q_block, 0)


def mix_kernel(meta, qs, rm, kn, kr, v, out, acc, total):
    def q_block(i, carry):
        pb, lo, hi = chunk_range(meta, i)
        rows = pl.ds(pl.multiple_of(i * BLK, BLK), BLK)
        acc[...] = jnp.zeros(acc.shape, jnp.float32)
        total[...] = jnp.zeros(total.shape, jnp.float32)

        def chunk(ch, carry):
            bias = bias_of(meta, pb, ch)
            keys = pl.ds(pl.multiple_of(ch * CHUNK, CHUNK), CHUNK)
            for h in range(4):
                s = scores_of(qs[h, rows, :], kn, kr, ch, h) + bias
                top = rm[h, rows, :]
                p0 = jnp.exp2((s[:, :128] - top) * (scale * math.log2(math.e)))
                p1 = jnp.exp2((s[:, 128:] - top) * (scale * math.log2(math.e)))
                total[h] += p0 + p1
                p = jnp.concatenate([p0, p1], axis=1).astype(jnp.bfloat16)
                acc[h] += jnp.dot(
                    p, v[keys, h * 128 : (h + 1) * 128], preferred_element_type=jnp.float32
                )
            return carry

        lax.fori_loop(lo, hi, chunk, 0)
        for h in range(4):
            whole = jnp.sum(total[h], axis=1, keepdims=True)
            out[rows, h * 128 : (h + 1) * 128] = (acc[h] / whole).astype(jnp.bfloat16)
        return carry

    lax.fori_loop(0, 4, q_block, 0)


def shift_seq(by):
    return [(i, (i + 2 * by) % 16) for i in range(16)]


SWAP = [(i, i ^ 1) for i in range(16)]
XSWAP = [(i, i ^ 4) for i in range(8)]


def shift_y(by):
    return [(x * 4 + y, x * 4 + (y + by) % 4) for x in range(2) for y in range(4)]


def ring(x):
    up, dn, got = x, x, [x]
    for s in range(4):
        up = lax.ppermute(up, "seq", shift_seq(1))
        got.append(up)
        if s < 3:
            dn = lax.ppermute(dn, "seq", shift_seq(-1))
            got.append(dn)
    return got


def swap(x):
    return lax.ppermute(x, "seq", SWAP)


def halves(w, c, width):
    mine = lax.dynamic_slice_in_dim(w, c * width, width, 1)
    other = swap(lax.dynamic_slice_in_dim(w, (1 - c) * width, width, 1))
    first = c == 0
    return jnp.concatenate([jnp.where(first, mine, other), jnp.where(first, other, mine)], axis=0)


def of_everyone(array, axis):
    copies = jnp.broadcast_to(array, (lax.axis_size(axis), *array.shape))
    return jnp.max(lax.all_to_all(copies, axis, split_axis=0, concat_axis=0, tiled=True), axis=0)


def on_device(query_latent, key_latent, rope_key, w_uq, w_uk, w_uv, block_order, segment_ids):
    bf16, f32 = jnp.bfloat16, jnp.float32
    s, t = lax.axis_index("seq"), lax.axis_index("tp")
    z, c, y, xl = s // 2, s % 2, t % 4, t // 4
    order, labels = block_order[0], segment_ids[0]
    bounds = jnp.stack([jnp.sum((labels < l).astype(jnp.int32)) for l in (1, 2, 3)])
    meta = jnp.concatenate(
        [order, bounds, jnp.stack([z, c, y, xl]).astype(jnp.int32), jnp.zeros((9,), jnp.int32)]
    )

    wq = halves(w_uq, c, 768)
    kv = halves(
        jnp.concatenate([w_uk[:, :512], w_uv[:, :512], w_uk[:, 512:], w_uv[:, 512:]], axis=1), c, 1024
    )
    chip = lax.dynamic_slice_in_dim(order, 4 * z, 4)
    chip = jnp.where(c == 0, chip, jnp.roll(chip, 2))
    pos = (chip[:, None] * BLK + jnp.arange(BLK, dtype=jnp.int32)[None, :]).reshape(-1)
    steps = jnp.arange(ROPE // 2, dtype=f32) * (2.0 / ROPE)
    freqs = jnp.exp(-math.log(rope_base) * steps)
    angle = pos.astype(f32)[:, None] * freqs[None, :]
    cos, sin = jnp.cos(angle), jnp.sin(angle)
    cs = jnp.concatenate([cos, cos, -sin, sin], axis=1)

    kq = jnp.concatenate([key_latent[0].T, query_latent[0].T], axis=0)
    kq_x = lax.ppermute(kq, "tp", XSWAP)
    k_x = jnp.concatenate([kq[:64], kq_x[:64]], axis=0).T
    q_x = jnp.concatenate([kq[64:], kq_x[64:]], axis=0).T
    rk = rope_key[0].astype(f32)
    a, b = rk[:, :32], rk[:, 32:]
    rc, rs = cos[:256], sin[:256]
    k_rope = jnp.concatenate([a * rc - b * rs, b * rc + a * rs], axis=1).astype(bf16)
    fold = jnp.concatenate([k_rope[:128], k_rope[128:]], axis=1)
    k_one = jnp.concatenate([k_x, lax.dynamic_slice_in_dim(fold, y * 32, 32, 0)], axis=0)

    k_ring = ring(k_one)
    kv_ring = ring(kv)
    w_ring = ring(wq)
    q_parts = [q_x] + [lax.ppermute(q_x, "tp", shift_y(by)) for by in (1, -1, 2)]
    q_own = jnp.concatenate(q_parts, axis=1)
    q_sib = swap(q_own)
    k_all = pl.pallas_call(
        join_kernel,
        out_shape=jax.ShapeDtypeStruct((8, 288, 128), bf16),
        in_specs=[VMEM] * 8,
        out_specs=VMEM,
        cost_estimate=pl.CostEstimate(flops=1 << 20, bytes_accessed=2 << 20, transcendentals=0),
        name="join",
    )(*k_ring)
    k_up = lax.ppermute(k_all, "tp", shift_y(1))
    k_dn = lax.ppermute(k_all, "tp", shift_y(-1))
    k_f1 = lax.ppermute(k_up[:4], "tp", shift_y(1))
    k_f2 = lax.ppermute(k_dn[4:], "tp", shift_y(-1))
    k_own = [k_all, k_up, k_dn, k_f1, k_f2]
    k_sib = [swap(p) for p in k_own]

    kn, v, kr = pl.pallas_call(
        project_kernel,
        out_shape=[
            jax.ShapeDtypeStruct((4096, 512), bf16),
            jax.ShapeDtypeStruct((4096, 512), bf16),
            jax.ShapeDtypeStruct((4096, 128), bf16),
        ],
        in_specs=[SMEM] + [ANY] * 18,
        out_specs=[VMEM] * 3,
        scratch_shapes=[
            pltpu.VMEM((16, 256, 512), bf16),
            pltpu.VMEM((16, 128, 128), bf16),
            pltpu.VMEM((512, 1024), bf16),
            pltpu.SemaphoreType.DMA((2, 5, 2)),
            pltpu.SemaphoreType.DMA((8,)),
        ],
        cost_estimate=pl.CostEstimate(
            flops=2 * 4096 * 512 * 1024, bytes_accessed=16 << 20, transcendentals=0
        ),
        name="project",
    )(meta, *k_own, *k_sib, *kv_ring)

    qs, rm, hm = pl.pallas_call(
        max_kernel,
        out_shape=[
            jax.ShapeDtypeStruct((4, 512, 256), bf16),
            jax.ShapeDtypeStruct((4, 512, 128), f32),
            jax.ShapeDtypeStruct((8, 128), f32),
        ],
        in_specs=[SMEM, VMEM, VMEM] + [ANY] * 8 + [VMEM] * 3,
        out_specs=[VMEM] * 3,
        scratch_shapes=[
            pltpu.VMEM((1536, 768), bf16),
            pltpu.SemaphoreType.DMA((8,)),
            pltpu.VMEM((4, 128, 128), f32),
        ],
        cost_estimate=pl.CostEstimate(
            flops=2 * 512 * 1536 * 768 + 2 * 512 * 2048 * 1024, bytes_accessed=12 << 20, transcendentals=0
        ),
        name="rowmax",
    )(meta, q_own, q_sib, *w_ring, cs, kn, kr)

    ctx = pl.pallas_call(
        mix_kernel,
        out_shape=jax.ShapeDtypeStruct((512, 512), bf16),
        in_specs=[SMEM] + [VMEM] * 5,
        out_specs=VMEM,
        scratch_shapes=[
            pltpu.VMEM((4, 128, 128), f32),
            pltpu.VMEM((4, 128, 128), f32),
        ],
        cost_estimate=pl.CostEstimate(
            flops=2 * 512 * 2048 * 2048, bytes_accessed=12 << 20, transcendentals=4 << 20
        ),
        name="mix",
    )(meta, qs, rm, kn, kr, v)

    local_max = hm[:4, 0]
    low = jnp.full((4,), masked_value, f32)
    both = jnp.where(
        c == 0, jnp.concatenate([local_max, low]), jnp.concatenate([low, local_max])
    )
    head_max = of_everyone(both, ("seq", "dp"))
    ratio = CLIP / jnp.maximum(head_max, CLIP)
    root = jnp.sqrt(ratio)
    factors = jnp.concatenate(
        [jnp.broadcast_to(root[:, None], (8, NOPE)), jnp.broadcast_to(ratio[:, None], (8, ROPE))], axis=1
    ).reshape(8 * (NOPE + ROPE))
    clipped_uq = (w_uq.astype(f32) * factors[None, :]).astype(bf16)
    clipped_uk = (w_uk.astype(f32) * jnp.repeat(root, NOPE)[None, :]).astype(bf16)

    got = swap(ctx[256:])
    own = ctx[:256]
    first = c == 0
    context = jnp.concatenate([jnp.where(first, own, got), jnp.where(first, got, own)], axis=1)
    return (context[None], clipped_uq, clipped_uk)


def solution(mesh):
    placed = (
        P("dp", "seq", "tp"),
        P("dp", "seq", "tp"),
        P("dp", "seq", None),
        P("seq", "tp"),
        P("seq", "tp"),
        P("seq", "tp"),
        P("dp", None),
        P("dp", None),
    )
    return jax.shard_map(
        on_device,
        mesh=mesh,
        in_specs=placed,
        out_specs=(P("dp", "seq", "tp"), P("seq", "tp"), P("seq", "tp")),
        check_vma=False,
    )
```

```python
import math

import jax
import jax.numpy as jnp
from jax import lax
from jax.experimental import pallas as pl
from jax.experimental.pallas import tpu as pltpu
from jax.sharding import PartitionSpec as P

NOPE = 128
ROPE = 64
VD = 128
CLIP = 8
BLK = 128
CHUNK = 256

rope_base = 50000.0
masked_value = -1e30
scale = 1.0 / math.sqrt(NOPE + ROPE)

ANY = pl.BlockSpec(memory_space=pl.ANY)
SMEM = pl.BlockSpec(memory_space=pltpu.SMEM)
VMEM = pl.BlockSpec(memory_space=pltpu.VMEM)


def meta_of(meta):
    return dict(z=meta[35], c=meta[36], y=meta[37], xl=meta[38])


def block_of(meta, i):
    m = meta_of(meta)
    half = i // 2
    core = jnp.where(half == 0, m["c"], 1 - m["c"])
    return meta[(m["z"] * 2 + core) * 2 + i % 2]


def start_of(meta, p):
    s = jnp.int32(0)
    for l in range(3):
        b = meta[32 + l]
        s = jnp.where(b <= p, jnp.maximum(s, b), s)
    return s


def feature_row(meta, t, each):
    m = meta_of(meta)
    x, yy = t // 4, t % 4
    dy = lax.rem(yy - m["y"] + 4, 4)
    j = jnp.where(dy == 0, 0, jnp.where(dy == 1, 2, jnp.where(dy == 2, 3, 1)))
    xr = jnp.where(x == m["xl"], 0, 1)
    return (j * 2 + xr) * each


RING = [0, -1, 1, -2, 2, -3, 3, -4]


def join_kernel(*refs):
    for j in range(8):
        refs[8][j] = refs[j][...]


def label_of(meta, p):
    label = jnp.zeros_like(p)
    for l in range(3):
        label = label + jnp.where(p >= meta[32 + l], 1, 0)
    return label


SLOTS = 38
EMPTY = 37
to_exp2 = scale * math.log2(math.e)


def attend_kernel(meta, *refs):
    q_in, w_in, kv_in, cs, pieces = refs[:2], refs[2:10], refs[10:18], refs[18], (refs[19:24], refs[24:29])
    out, hm = refs[29:31]
    q, w, kvw, lat, rope, kn, v, kr, qs, sbuf, mx, rm, acc, total, step_i, step_ch, need = refs[31:48]
    qsem, wsem, kvsem, ksem = refs[48:]
    m = meta_of(meta)
    f32, bf16 = jnp.float32, jnp.bfloat16
    first, second = [], []
    for half in range(2):
        first.append(pltpu.make_async_copy(q_in[half], q.at[half], qsem.at[half]))
    for j in range(8):
        t = lax.rem(m["z"] + RING[j] + 8, 8)
        row = pl.multiple_of(feature_row(meta, t, 192), 64)
        first.append(pltpu.make_async_copy(w_in[j], w.at[pl.ds(row, 192)], wsem.at[j]))
        row = pl.multiple_of(feature_row(meta, t, 64), 64)
        second.append(pltpu.make_async_copy(kv_in[j], kvw.at[pl.ds(row, 64)], kvsem.at[j]))
    for core in range(2):
        own, up, dn, f1, f2 = pieces[core]
        for n, (src, plane, start, count, dy) in enumerate(
            ((own, 0, 0, 8, 0), (up, 1, 0, 8, 3), (dn, 2, 0, 8, 1), (f1, 3, 0, 4, 2), (f2, 3, 4, 4, 2))
        ):
            rows = pl.ds(core * 8 + start, count)
            yq = pl.multiple_of(lax.rem(m["y"] + dy, 4) * 32, 32)
            second.append(
                pltpu.make_async_copy(src.at[:, :256, :], lat.at[plane, rows], ksem.at[core, n, 0])
            )
            second.append(
                pltpu.make_async_copy(
                    src.at[:, 256:, :], rope.at[rows, pl.ds(yq, 32), :], ksem.at[core, n, 1]
                )
            )
    for cp in first + second:
        cp.start()

    for n in range(16):
        need[n] = 0
    count = jnp.int32(0)
    for i in range(4):
        pb = block_of(meta, i)
        lo = start_of(meta, pb * BLK) // CHUNK
        hi = pb // 2
        need[hi] = 1

        def add(ch, g, i=i):
            step_i[g] = i
            step_ch[g] = ch
            need[ch] = 1
            return g + 1

        count = lax.fori_loop(lo, hi, add, count)
    step_i[count] = 3
    step_ch[count] = block_of(meta, 3) // 2
    odd = lax.rem(count, 2)

    lane64 = lax.broadcasted_iota(jnp.int32, (BLK, 64), 1)
    row64 = lax.broadcasted_iota(jnp.int32, (BLK, 64), 0)
    for cp in first:
        cp.wait()
    for half in range(2):
        full = jnp.dot(q[half], w[...], preferred_element_type=f32)
        labels = [
            jnp.where(label_of(meta, row64 + block_of(meta, half * 2 + b) * BLK) == lane64, 1.0, 0.0)
            for b in range(2)
        ]
        onehot = jnp.concatenate(labels, axis=0).astype(bf16)
        rows = slice(half * 256, half * 256 + 256)
        cos = cs[rows, :64]
        sin = cs[rows, 64:]
        for h in range(4):
            nope = full[:, h * 192 : h * 192 + 128].astype(bf16)
            r = full[:, h * 192 + 128 : h * 192 + 192]
            turned = jnp.concatenate([r[:, 32:], r[:, :32]], axis=1)
            rot = (r * cos + turned * sin).astype(bf16)
            qs[h, rows, :128] = nope
            qs[h, rows, 128:] = jnp.concatenate([rot, onehot], axis=1)

    mx[...] = jnp.full(mx.shape, masked_value, f32)
    acc[...] = jnp.zeros(acc.shape, f32)
    total[...] = jnp.zeros(total.shape, f32)
    sbuf[EMPTY] = jnp.full((4, BLK, CHUNK), masked_value, f32)
    for cp in second:
        cp.wait()

    def project(i, carry):
        j = lax.rem(i, 8)
        s = (j + 1) // 2
        dz = jnp.where(lax.rem(j, 2) == 1, -s, s)
        zz = lax.rem(m["z"] + dz + 8, 8)
        cc = jnp.where(i < 8, m["c"], 1 - m["c"])
        base = (zz * 2 + cc) * 2

        @pl.when((need[meta[base] // 2] + need[meta[base + 1] // 2]) > 0)
        def _():
            x = jnp.concatenate([lat[n, i] for n in range(4)], axis=1)
            y = jnp.dot(x, kvw[...], preferred_element_type=f32)
            fold = rope[i]
            for b in range(2):
                pb = pl.multiple_of(meta[base + b] * BLK, BLK)
                rows = slice(b * BLK, (b + 1) * BLK)
                kn[pl.ds(pb, BLK), :] = y[rows, :512].astype(bf16)
                v[pl.ds(pb, BLK), :] = y[rows, 512:].astype(bf16)
                label = label_of(meta, row64 + pb)
                apart = jnp.where((lane64 < 4) & (lane64 != label), masked_value, 0.0).astype(bf16)
                kr[pl.ds(pb, BLK), :] = jnp.concatenate(
                    [fold[:, b * 64 : b * 64 + 64], apart], axis=1
                )

        return carry

    lax.fori_loop(0, 16, project, 0)

    def scores(i, ch):
        keys = pl.ds(pl.multiple_of(ch * CHUNK, CHUNK), CHUNK)
        rows = pl.ds(pl.multiple_of(i * BLK, BLK), BLK)
        got = []
        for h in range(4):
            k = jnp.concatenate([kn[keys, h * 128 : (h + 1) * 128], kr[keys, :]], axis=1)
            got.append(
                lax.dot_general(
                    qs[h, rows, :], k, (((1,), (1,)), ((), ())), preferred_element_type=f32
                )
            )
        return got

    def keep(i, slot, h, s):
        sbuf[slot, h] = s
        mx[i, h] = jnp.maximum(mx[i, h], jnp.maximum(s[:, :128], s[:, 128:]))

    def diagonal(i, carry):
        pb = block_of(meta, i)
        ch = pb // 2
        row = lax.broadcasted_iota(jnp.int32, (BLK, CHUNK), 0) + (pb * BLK - ch * CHUNK)
        col = lax.broadcasted_iota(jnp.int32, (BLK, CHUNK), 1)
        bias = jnp.where(col <= row, 0.0, masked_value)
        for h, s in enumerate(scores(i, ch)):
            keep(i, i, h, s + bias)
        return carry

    lax.fori_loop(0, 4, diagonal, 0)

    def score_pair(n, carry):
        picks = []
        for g in (2 * n, jnp.minimum(2 * n + 1, count - 1)):
            i, ch = step_i[g], step_ch[g]
            picks.append((i, g + 4, scores(i, ch)))
        for i, slot, got in picks:
            for h, s in enumerate(got):
                keep(i, slot, h, s)
        return carry

    pairs = (count + odd) // 2
    lax.fori_loop(0, pairs, score_pair, 0)

    hm[...] = jnp.full(hm.shape, masked_value, f32)

    def finish_max(i, carry):
        for h in range(4):
            top = jnp.broadcast_to(jnp.max(mx[i, h], axis=1, keepdims=True), (BLK, 128))
            rm[i, h] = top * to_exp2
            best = jnp.max(top, axis=0, keepdims=True) * scale
            hm[h : h + 1, :] = jnp.maximum(hm[h : h + 1, :], best)
        return carry

    lax.fori_loop(0, 4, finish_max, 0)

    def mix(steps):
        for i, ch, slot in steps:
            keys = pl.ds(pl.multiple_of(ch * CHUNK, CHUNK), CHUNK)
            for h in range(4):
                s = sbuf[slot, h]
                top = rm[i, h]
                p0 = jnp.exp2(s[:, :128] * to_exp2 - top)
                p1 = jnp.exp2(s[:, 128:] * to_exp2 - top)
                total[i, h] += p0 + p1
                p = jnp.concatenate([p0, p1], axis=1).astype(bf16)
                acc[i, h] += jnp.dot(p, v[keys, h * 128 : (h + 1) * 128], preferred_element_type=f32)

    def mix_diagonal(n, carry):
        mix([(2 * n + e, block_of(meta, 2 * n + e) // 2, 2 * n + e) for e in range(2)])
        return carry

    lax.fori_loop(0, 2, mix_diagonal, 0)

    def mix_pair(n, carry):
        a, b = 2 * n, 2 * n + 1
        slot = jnp.where(b < count, b + 4, EMPTY)
        mix([(step_i[a], step_ch[a], a + 4), (step_i[b], step_ch[b], slot)])
        return carry

    lax.fori_loop(0, pairs, mix_pair, 0)

    def finish(i, carry):
        rows = pl.ds(pl.multiple_of(i * BLK, BLK), BLK)
        for h in range(4):
            whole = jnp.sum(total[i, h], axis=1, keepdims=True)
            out[rows, h * 128 : (h + 1) * 128] = (acc[i, h] / whole).astype(bf16)
        return carry

    lax.fori_loop(0, 4, finish, 0)


def shift_seq(by):
    return [(i, (i + 2 * by) % 16) for i in range(16)]


SWAP = [(i, i ^ 1) for i in range(16)]
XSWAP = [(i, i ^ 4) for i in range(8)]


def shift_y(by):
    return [(x * 4 + y, x * 4 + (y + by) % 4) for x in range(2) for y in range(4)]


def ring(x):
    up, dn, got = x, x, [x]
    for s in range(4):
        up = lax.ppermute(up, "seq", shift_seq(1))
        got.append(up)
        if s < 3:
            dn = lax.ppermute(dn, "seq", shift_seq(-1))
            got.append(dn)
    return got


def swap(x):
    return lax.ppermute(x, "seq", SWAP)


def halves(w, c, width):
    mine = lax.dynamic_slice_in_dim(w, c * width, width, 1)
    other = swap(lax.dynamic_slice_in_dim(w, (1 - c) * width, width, 1))
    first = c == 0
    return jnp.concatenate([jnp.where(first, mine, other), jnp.where(first, other, mine)], axis=0)


def of_everyone(array, axis):
    copies = jnp.broadcast_to(array, (lax.axis_size(axis), *array.shape))
    return jnp.max(lax.all_to_all(copies, axis, split_axis=0, concat_axis=0, tiled=True), axis=0)


def on_device(query_latent, key_latent, rope_key, w_uq, w_uk, w_uv, block_order, segment_ids):
    bf16, f32 = jnp.bfloat16, jnp.float32
    s, t = lax.axis_index("seq"), lax.axis_index("tp")
    z, c, y, xl = s // 2, s % 2, t % 4, t // 4
    order, labels = block_order[0], segment_ids[0]
    bounds = jnp.stack([jnp.sum((labels < l).astype(jnp.int32)) for l in (1, 2, 3)])
    meta = jnp.concatenate(
        [order, bounds, jnp.stack([z, c, y, xl]).astype(jnp.int32), jnp.zeros((9,), jnp.int32)]
    )

    wq = halves(w_uq, c, 768)
    kv = halves(
        jnp.concatenate([w_uk[:, :512], w_uv[:, :512], w_uk[:, 512:], w_uv[:, 512:]], axis=1), c, 1024
    )
    chip = lax.dynamic_slice_in_dim(order, 4 * z, 4)
    chip = jnp.where(c == 0, chip, jnp.roll(chip, 2))
    pos = (chip[:, None] * BLK + jnp.arange(BLK, dtype=jnp.int32)[None, :]).reshape(-1)
    steps = jnp.arange(ROPE // 2, dtype=f32) * (2.0 / ROPE)
    freqs = jnp.exp(-math.log(rope_base) * steps)
    angle = pos.astype(f32)[:, None] * freqs[None, :]
    cos, sin = jnp.cos(angle), jnp.sin(angle)
    cs = jnp.concatenate([cos, cos, -sin, sin], axis=1)

    kq = jnp.concatenate([key_latent[0].T, query_latent[0].T], axis=0)
    kq_x = lax.ppermute(kq, "tp", XSWAP)
    k_x = jnp.concatenate([kq[:64], kq_x[:64]], axis=0).T
    q_x = jnp.concatenate([kq[64:], kq_x[64:]], axis=0).T
    rk = rope_key[0].astype(f32)
    a, b = rk[:, :32], rk[:, 32:]
    rc, rs = cos[:256], sin[:256]
    k_rope = jnp.concatenate([a * rc - b * rs, b * rc + a * rs], axis=1).astype(bf16)
    fold = jnp.concatenate([k_rope[:128], k_rope[128:]], axis=1)
    k_one = jnp.concatenate([k_x, lax.dynamic_slice_in_dim(fold, y * 32, 32, 0)], axis=0)

    k_ring = ring(k_one)
    kv_ring = ring(kv)
    w_ring = ring(wq)
    q_parts = [q_x] + [lax.ppermute(q_x, "tp", shift_y(by)) for by in (1, -1, 2)]
    q_own = jnp.concatenate(q_parts, axis=1)
    q_sib = swap(q_own)
    k_all = pl.pallas_call(
        join_kernel,
        out_shape=jax.ShapeDtypeStruct((8, 288, 128), bf16),
        in_specs=[VMEM] * 8,
        out_specs=VMEM,
        cost_estimate=pl.CostEstimate(flops=1 << 20, bytes_accessed=2 << 20, transcendentals=0),
        name="join",
    )(*k_ring)
    k_up = lax.ppermute(k_all, "tp", shift_y(1))
    k_dn = lax.ppermute(k_all, "tp", shift_y(-1))
    k_f1 = lax.ppermute(k_up[:4], "tp", shift_y(1))
    k_f2 = lax.ppermute(k_dn[4:], "tp", shift_y(-1))
    k_own = [k_all, k_up, k_dn, k_f1, k_f2]
    k_sib = [swap(p) for p in k_own]

    vm = pltpu.VMEM
    ctx, hm = pl.pallas_call(
        attend_kernel,
        out_shape=[
            jax.ShapeDtypeStruct((512, 512), bf16),
            jax.ShapeDtypeStruct((8, 128), f32),
        ],
        in_specs=[SMEM] + [ANY] * 18 + [VMEM] + [ANY] * 10,
        out_specs=[VMEM] * 2,
        scratch_shapes=[
            vm((2, 256, 1536), bf16),
            vm((1536, 768), bf16),
            vm((512, 1024), bf16),
            vm((4, 16, 256, 128), bf16),
            vm((16, 128, 128), bf16),
            vm((4096, 512), bf16),
            vm((4096, 512), bf16),
            vm((4096, 128), bf16),
            vm((4, 512, 256), bf16),
            vm((SLOTS, 4, BLK, CHUNK), f32),
            vm((4, 4, BLK, 128), f32),
            vm((4, 4, BLK, 128), f32),
            vm((4, 4, BLK, 128), f32),
            vm((4, 4, BLK, 128), f32),
            pltpu.SMEM((40,), jnp.int32),
            pltpu.SMEM((40,), jnp.int32),
            pltpu.SMEM((16,), jnp.int32),
            pltpu.SemaphoreType.DMA((2,)),
            pltpu.SemaphoreType.DMA((8,)),
            pltpu.SemaphoreType.DMA((8,)),
            pltpu.SemaphoreType.DMA((2, 5, 2)),
        ],
        compiler_params=pltpu.CompilerParams(vmem_limit_bytes=60 << 20),
        cost_estimate=pl.CostEstimate(
            flops=20 << 30, bytes_accessed=12 << 20, transcendentals=4 << 20
        ),
        name="attend",
    )(meta, q_own, q_sib, *w_ring, *kv_ring, cs, *k_own, *k_sib)

    local_max = hm[:4, 0]
    low = jnp.full((4,), masked_value, f32)
    both = jnp.where(
        c == 0, jnp.concatenate([local_max, low]), jnp.concatenate([low, local_max])
    )
    head_max = of_everyone(both, ("seq", "dp"))
    ratio = CLIP / jnp.maximum(head_max, CLIP)
    root = jnp.sqrt(ratio)
    factors = jnp.concatenate(
        [jnp.broadcast_to(root[:, None], (8, NOPE)), jnp.broadcast_to(ratio[:, None], (8, ROPE))], axis=1
    ).reshape(8 * (NOPE + ROPE))
    clipped_uq = (w_uq.astype(f32) * factors[None, :]).astype(bf16)
    clipped_uk = (w_uk.astype(f32) * jnp.repeat(root, NOPE)[None, :]).astype(bf16)

    got = swap(ctx[256:])
    own = ctx[:256]
    first = c == 0
    context = jnp.concatenate([jnp.where(first, own, got), jnp.where(first, got, own)], axis=1)
    return (context[None], clipped_uq, clipped_uk)


def solution(mesh):
    placed = (
        P("dp", "seq", "tp"),
        P("dp", "seq", "tp"),
        P("dp", "seq", None),
        P("seq", "tp"),
        P("seq", "tp"),
        P("seq", "tp"),
        P("dp", None),
        P("dp", None),
    )
    return jax.shard_map(
        on_device,
        mesh=mesh,
        in_specs=placed,
        out_specs=(P("dp", "seq", "tp"), P("seq", "tp"), P("seq", "tp")),
        check_vma=False,
    )
```

```python
import math

import jax
import jax.numpy as jnp
from jax import lax
from jax.experimental import pallas as pl
from jax.experimental.pallas import tpu as pltpu
from jax.sharding import PartitionSpec as P

NOPE = 128
ROPE = 64
VD = 128
CLIP = 8
BLK = 128
CHUNK = 256

rope_base = 50000.0
masked_value = -1e30
scale = 1.0 / math.sqrt(NOPE + ROPE)

ANY = pl.BlockSpec(memory_space=pl.ANY)
SMEM = pl.BlockSpec(memory_space=pltpu.SMEM)
VMEM = pl.BlockSpec(memory_space=pltpu.VMEM)


def where_am_i():
    s, t = lax.axis_index("seq"), lax.axis_index("tp")
    return dict(z=s // 2, c=lax.rem(s, 2), y=lax.rem(t, 4), xl=t // 4)


def start_of(bounds, p):
    s = jnp.int32(0)
    for b in bounds:
        s = jnp.where(b <= p, jnp.maximum(s, b), s)
    return s


def feature_row(m, t, each):
    x, yy = t // 4, t % 4
    dy = lax.rem(yy - m["y"] + 4, 4)
    j = jnp.where(dy == 0, 0, jnp.where(dy == 1, 2, jnp.where(dy == 2, 3, 1)))
    xr = jnp.where(x == m["xl"], 0, 1)
    return (j * 2 + xr) * each


RING = [0, -1, 1, -2, 2, -3, 3, -4]


def split_kernel(q_t, k_t, w_uq, w_uk, w_uv, kq, w_mine, w_send, kv_mine, kv_send):
    c = where_am_i()["c"]
    kq[:64] = k_t[...]
    kq[64:] = q_t[...]

    def halves(own):
        other = 1 - own
        w_mine[...] = w_uq[:, own * 768 : own * 768 + 768]
        w_send[...] = w_uq[:, other * 768 : other * 768 + 768]
        for n in range(4):
            for to, half in ((kv_mine, own), (kv_send, other)):
                cols = slice(half * 512 + n * 128, half * 512 + n * 128 + 128)
                to[n] = w_uk[:, cols]
                to[4 + n] = w_uv[:, cols]

    @pl.when(c == 0)
    def _():
        halves(0)

    @pl.when(c == 1)
    def _():
        halves(1)


def turn_kernel(order, rope_t, cs, share, fold):
    m = where_am_i()
    pos = []
    lane = lax.broadcasted_iota(jnp.int32, (32, BLK), 1)
    for i in range(4):
        core = m["c"] if i < 2 else 1 - m["c"]
        pos.append(lane + order[0, (m["z"] * 2 + core) * 2 + i % 2] * BLK)
    steps = lax.broadcasted_iota(jnp.int32, (32, 512), 0).astype(jnp.float32) * (2.0 / ROPE)
    freqs = jnp.exp(-math.log(rope_base) * steps)
    angle = jnp.concatenate(pos, axis=1).astype(jnp.float32) * freqs
    cos, sin = jnp.cos(angle), jnp.sin(angle)
    cs[...] = jnp.concatenate([cos, cos, -sin, sin], axis=0).T
    r = rope_t[...].astype(jnp.float32)
    a, b, rc, rs = r[:32], r[32:], cos[:, :256], sin[:, :256]
    both = jnp.concatenate([a * rc - b * rs, b * rc + a * rs], axis=0)
    fold[...] = jnp.concatenate([both[:, :128], both[:, 128:]], axis=0).T.astype(jnp.bfloat16)
    share[...] = fold[pl.ds(pl.multiple_of(m["y"] * 32, 32), 32), :]


def rows_kernel(w_mine, w_other, wq):
    c = where_am_i()["c"]
    wq[pl.ds(pl.multiple_of(c * 96, 32), 96), :] = w_mine[...]
    wq[pl.ds(pl.multiple_of((1 - c) * 96, 32), 96), :] = w_other[...]


def pack_kernel(kq, kq_x, share, kv_mine, kv_other, k_one, q_x):
    c = where_am_i()["c"]
    k_one[:256] = jnp.concatenate([kq[:64], kq_x[:64]], axis=0).T
    k_one[256:288] = share[...]
    for n in range(8):
        k_one[pl.ds(pl.multiple_of(288 + n * 64 + c * 32, 32), 32), :] = kv_mine[n]
        k_one[pl.ds(pl.multiple_of(288 + n * 64 + (1 - c) * 32, 32), 32), :] = kv_other[n]
    q_x[...] = jnp.concatenate([kq[64:], kq_x[64:]], axis=0).T


def join_kernel(*refs):
    ins, out, sem = refs[:8], refs[8], refs[9]
    copies = [pltpu.make_async_copy(r.at[:288], out.at[j], sem.at[j]) for j, r in enumerate(ins)]
    for cp in copies:
        cp.start()
    for cp in copies:
        cp.wait()


def label_of(bounds, p):
    label = jnp.zeros_like(p)
    for b in bounds:
        label = label + jnp.where(p >= b, 1, 0)
    return label


SLOTS = 38
EMPTY = 37
to_exp2 = scale * math.log2(math.e)


def attend_kernel(order, seg, *refs):
    q_in, w_in, kv_in, cs, pieces = refs[:2], refs[2:10], refs[10:18], refs[18], (refs[19:24], refs[24:29])
    out, hm = refs[29:31]
    q, w, kvw, lat, rope, kn, v, kr, qs, sbuf, mx, rm, acc, total, step_i, step_ch, need = refs[31:48]
    qsem, wsem, kvsem, ksem = refs[48:]
    m = where_am_i()

    def block_of(i):
        core = jnp.where(i // 2 == 0, m["c"], 1 - m["c"])
        return order[0, (m["z"] * 2 + core) * 2 + lax.rem(i, 2)]

    f32, bf16 = jnp.float32, jnp.bfloat16
    first, second = [], []
    for half in range(2):
        first.append(pltpu.make_async_copy(q_in[half], q.at[half], qsem.at[half]))
    for j in range(8):
        t = lax.rem(m["z"] + RING[j] + 8, 8)
        row = pl.multiple_of(feature_row(m, t, 192), 64)
        first.append(pltpu.make_async_copy(w_in[j], w.at[pl.ds(row, 192)], wsem.at[j]))
        row = pl.multiple_of(feature_row(m, t, 64), 64)
        for n in range(8):
            second.append(
                pltpu.make_async_copy(
                    kv_in[j].at[pl.ds(288 + n * 64, 64)],
                    kvw.at[pl.ds(row, 64), pl.ds(n * 128, 128)],
                    kvsem.at[j, n],
                )
            )
    for core in range(2):
        own, up, dn, f1, f2 = pieces[core]
        for n, (src, plane, start, count, dy) in enumerate(
            ((own, 0, 0, 8, 0), (up, 1, 0, 8, 3), (dn, 2, 0, 8, 1), (f1, 3, 0, 4, 2), (f2, 3, 4, 4, 2))
        ):
            rows = pl.ds(core * 8 + start, count)
            yq = pl.multiple_of(lax.rem(m["y"] + dy, 4) * 32, 32)
            second.append(
                pltpu.make_async_copy(src.at[:, :256, :], lat.at[plane, rows], ksem.at[core, n, 0])
            )
            second.append(
                pltpu.make_async_copy(
                    src.at[:, 256:, :], rope.at[rows, pl.ds(yq, 32), :], ksem.at[core, n, 1]
                )
            )
    for cp in first + second:
        cp.start()

    bounds = [jnp.sum(jnp.where(seg[...] < l, 1, 0)) for l in (1, 2, 3)]

    for n in range(16):
        need[n] = 0
    count = jnp.int32(0)
    for i in range(4):
        pb = block_of(i)
        lo = start_of(bounds, pb * BLK) // CHUNK
        hi = pb // 2
        need[hi] = 1

        def add(ch, g, i=i):
            step_i[g] = i
            step_ch[g] = ch
            need[ch] = 1
            return g + 1

        count = lax.fori_loop(lo, hi, add, count)
    step_i[count] = 3
    step_ch[count] = block_of(3) // 2
    odd = lax.rem(count, 2)

    lane64 = lax.broadcasted_iota(jnp.int32, (BLK, 64), 1)
    row64 = lax.broadcasted_iota(jnp.int32, (BLK, 64), 0)
    for cp in first:
        cp.wait()
    for half in range(2):
        full = jnp.dot(q[half], w[...], preferred_element_type=f32)
        labels = [
            jnp.where(label_of(bounds, row64 + block_of(half * 2 + b) * BLK) == lane64, 1.0, 0.0)
            for b in range(2)
        ]
        onehot = jnp.concatenate(labels, axis=0).astype(bf16)
        rows = slice(half * 256, half * 256 + 256)
        cos = cs[rows, :64]
        sin = cs[rows, 64:]
        for h in range(4):
            nope = full[:, h * 192 : h * 192 + 128].astype(bf16)
            r = full[:, h * 192 + 128 : h * 192 + 192]
            turned = jnp.concatenate([r[:, 32:], r[:, :32]], axis=1)
            rot = (r * cos + turned * sin).astype(bf16)
            qs[h, rows, :128] = nope
            qs[h, rows, 128:] = jnp.concatenate([rot, onehot], axis=1)

    mx[...] = jnp.full(mx.shape, masked_value, f32)
    acc[...] = jnp.zeros(acc.shape, f32)
    total[...] = jnp.zeros(total.shape, f32)
    sbuf[EMPTY] = jnp.full((4, BLK, CHUNK), masked_value, f32)
    for cp in second:
        cp.wait()

    def project(i, carry):
        j = lax.rem(i, 8)
        s = (j + 1) // 2
        dz = jnp.where(lax.rem(j, 2) == 1, -s, s)
        zz = lax.rem(m["z"] + dz + 8, 8)
        cc = jnp.where(i < 8, m["c"], 1 - m["c"])
        base = (zz * 2 + cc) * 2

        @pl.when((need[order[0, base] // 2] + need[order[0, base + 1] // 2]) > 0)
        def _():
            x = jnp.concatenate([lat[n, i] for n in range(4)], axis=1)
            y = jnp.dot(x, kvw[...], preferred_element_type=f32)
            fold = rope[i]
            for b in range(2):
                pb = pl.multiple_of(order[0, base + b] * BLK, BLK)
                rows = slice(b * BLK, (b + 1) * BLK)
                kn[pl.ds(pb, BLK), :] = y[rows, :512].astype(bf16)
                v[pl.ds(pb, BLK), :] = y[rows, 512:].astype(bf16)
                label = label_of(bounds, row64 + pb)
                apart = jnp.where((lane64 < 4) & (lane64 != label), masked_value, 0.0).astype(bf16)
                kr[pl.ds(pb, BLK), :] = jnp.concatenate(
                    [fold[:, b * 64 : b * 64 + 64], apart], axis=1
                )

        return carry

    lax.fori_loop(0, 16, project, 0)

    def scores(i, ch):
        keys = pl.ds(pl.multiple_of(ch * CHUNK, CHUNK), CHUNK)
        rows = pl.ds(pl.multiple_of(i * BLK, BLK), BLK)
        got = []
        for h in range(4):
            k = jnp.concatenate([kn[keys, h * 128 : (h + 1) * 128], kr[keys, :]], axis=1)
            got.append(
                lax.dot_general(
                    qs[h, rows, :], k, (((1,), (1,)), ((), ())), preferred_element_type=f32
                )
            )
        return got

    def keep(i, slot, h, s):
        sbuf[slot, h] = s
        mx[i, h] = jnp.maximum(mx[i, h], jnp.maximum(s[:, :128], s[:, 128:]))

    def diagonal(i, carry):
        pb = block_of(i)
        ch = pb // 2
        row = lax.broadcasted_iota(jnp.int32, (BLK, CHUNK), 0) + (pb * BLK - ch * CHUNK)
        col = lax.broadcasted_iota(jnp.int32, (BLK, CHUNK), 1)
        bias = jnp.where(col <= row, 0.0, masked_value)
        for h, s in enumerate(scores(i, ch)):
            keep(i, i, h, s + bias)
        return carry

    lax.fori_loop(0, 4, diagonal, 0)

    def score_pair(n, carry):
        picks = []
        for g in (2 * n, jnp.minimum(2 * n + 1, count - 1)):
            i, ch = step_i[g], step_ch[g]
            picks.append((i, g + 4, scores(i, ch)))
        for i, slot, got in picks:
            for h, s in enumerate(got):
                keep(i, slot, h, s)
        return carry

    pairs = (count + odd) // 2
    lax.fori_loop(0, pairs, score_pair, 0)

    hm[...] = jnp.full(hm.shape, masked_value, f32)

    def finish_max(i, carry):
        for h in range(4):
            top = jnp.broadcast_to(jnp.max(mx[i, h], axis=1, keepdims=True), (BLK, 128))
            rm[i, h] = top * to_exp2
            best = jnp.max(top, axis=0, keepdims=True) * scale
            hm[h : h + 1, :] = jnp.maximum(hm[h : h + 1, :], best)
        return carry

    lax.fori_loop(0, 4, finish_max, 0)

    def mix(steps):
        for i, ch, slot in steps:
            keys = pl.ds(pl.multiple_of(ch * CHUNK, CHUNK), CHUNK)
            for h in range(4):
                s = sbuf[slot, h]
                top = rm[i, h]
                p0 = jnp.exp2(s[:, :128] * to_exp2 - top)
                p1 = jnp.exp2(s[:, 128:] * to_exp2 - top)
                total[i, h] += p0 + p1
                p = jnp.concatenate([p0, p1], axis=1).astype(bf16)
                acc[i, h] += jnp.dot(p, v[keys, h * 128 : (h + 1) * 128], preferred_element_type=f32)

    def mix_diagonal(n, carry):
        mix([(2 * n + e, block_of(2 * n + e) // 2, 2 * n + e) for e in range(2)])
        return carry

    lax.fori_loop(0, 2, mix_diagonal, 0)

    def mix_pair(n, carry):
        a, b = 2 * n, 2 * n + 1
        slot = jnp.where(b < count, b + 4, EMPTY)
        mix([(step_i[a], step_ch[a], a + 4), (step_i[b], step_ch[b], slot)])
        return carry

    lax.fori_loop(0, pairs, mix_pair, 0)

    def finish(i, carry):
        rows = pl.ds(pl.multiple_of(i * BLK, BLK), BLK)
        for h in range(4):
            whole = jnp.sum(total[i, h], axis=1, keepdims=True)
            out[rows, h * 128 : (h + 1) * 128] = (acc[i, h] / whole).astype(bf16)
        return carry

    lax.fori_loop(0, 4, finish, 0)


def shift_seq(by):
    return [(i, (i + 2 * by) % 16) for i in range(16)]


SWAP = [(i, i ^ 1) for i in range(16)]
XSWAP = [(i, i ^ 4) for i in range(8)]


def shift_y(by):
    return [(x * 4 + y, x * 4 + (y + by) % 4) for x in range(2) for y in range(4)]


def ring(x):
    up, dn, got = x, x, [x]
    for s in range(4):
        up = lax.ppermute(up, "seq", shift_seq(1))
        got.append(up)
        if s < 3:
            dn = lax.ppermute(dn, "seq", shift_seq(-1))
            got.append(dn)
    return got


def swap(x):
    return lax.ppermute(x, "seq", SWAP)


def call(kernel, outs, args, specs=None, scratch=(), name=None):
    outs = [jax.ShapeDtypeStruct(shape, dtype) for shape, dtype in outs]
    size = sum(math.prod(o.shape) * o.dtype.itemsize for o in outs)
    return pl.pallas_call(
        kernel,
        out_shape=outs,
        in_specs=specs or [VMEM] * len(args),
        out_specs=[VMEM] * len(outs),
        scratch_shapes=list(scratch),
        cost_estimate=pl.CostEstimate(flops=1 << 20, bytes_accessed=2 * size, transcendentals=0),
        name=name,
    )(*args)


def of_everyone(array, axis):
    copies = jnp.broadcast_to(array, (lax.axis_size(axis), *array.shape))
    return jnp.max(lax.all_to_all(copies, axis, split_axis=0, concat_axis=0, tiled=True), axis=0)


def on_device(query_latent, key_latent, rope_key, w_uq, w_uk, w_uv, block_order, segment_ids):
    bf16, f32 = jnp.bfloat16, jnp.float32
    c = where_am_i()["c"]
    kq, w_mine, w_send, kv_mine, kv_send = call(
        split_kernel,
        [((256, 256), bf16)] + [((96, 768), bf16)] * 2 + [((8, 32, 128), bf16)] * 2,
        (query_latent[0].T, key_latent[0].T, w_uq, w_uk, w_uv),
        name="split",
    )
    kq_x = lax.ppermute(kq, "tp", XSWAP)
    w_other = swap(w_send)
    kv_other = swap(kv_send)
    cs, share = call(
        turn_kernel,
        [((512, 128), f32), ((32, 128), bf16)],
        (block_order, rope_key[0].T),
        specs=[SMEM, VMEM],
        scratch=[pltpu.VMEM((128, 128), bf16)],
        name="turn",
    )
    (wq,) = call(rows_kernel, [((192, 768), bf16)], (w_mine, w_other), name="rows")
    k_one, q_x = call(
        pack_kernel,
        [((800, 128), bf16), ((256, 384), bf16)],
        (kq, kq_x, share, kv_mine, kv_other),
        name="pack",
    )

    w_ring = ring(wq)
    k_ring = ring(k_one)
    q_parts = [q_x] + [lax.ppermute(q_x, "tp", shift_y(by)) for by in (1, -1, 2)]
    q_own = jnp.concatenate(q_parts, axis=1)
    q_sib = swap(q_own)
    (k_all,) = call(
        join_kernel,
        [((8, 288, 128), bf16)],
        k_ring,
        specs=[ANY] * 8,
        scratch=[pltpu.SemaphoreType.DMA((8,))],
        name="join",
    )
    k_up = lax.ppermute(k_all, "tp", shift_y(1))
    k_dn = lax.ppermute(k_all, "tp", shift_y(-1))
    k_f1 = lax.ppermute(k_up[:4], "tp", shift_y(1))
    k_f2 = lax.ppermute(k_dn[4:], "tp", shift_y(-1))
    k_own = [k_all, k_up, k_dn, k_f1, k_f2]
    k_sib = [swap(p) for p in k_own]

    vm = pltpu.VMEM
    ctx, hm = pl.pallas_call(
        attend_kernel,
        out_shape=[
            jax.ShapeDtypeStruct((512, 512), bf16),
            jax.ShapeDtypeStruct((8, 128), f32),
        ],
        in_specs=[SMEM, VMEM] + [ANY] * 18 + [VMEM] + [ANY] * 10,
        out_specs=[VMEM] * 2,
        scratch_shapes=[
            vm((2, 256, 1536), bf16),
            vm((1536, 768), bf16),
            vm((512, 1024), bf16),
            vm((4, 16, 256, 128), bf16),
            vm((16, 128, 128), bf16),
            vm((4096, 512), bf16),
            vm((4096, 512), bf16),
            vm((4096, 128), bf16),
            vm((4, 512, 256), bf16),
            vm((SLOTS, 4, BLK, CHUNK), f32),
            vm((4, 4, BLK, 128), f32),
            vm((4, 4, BLK, 128), f32),
            vm((4, 4, BLK, 128), f32),
            vm((4, 4, BLK, 128), f32),
            pltpu.SMEM((40,), jnp.int32),
            pltpu.SMEM((40,), jnp.int32),
            pltpu.SMEM((16,), jnp.int32),
            pltpu.SemaphoreType.DMA((2,)),
            pltpu.SemaphoreType.DMA((8,)),
            pltpu.SemaphoreType.DMA((8, 8)),
            pltpu.SemaphoreType.DMA((2, 5, 2)),
        ],
        compiler_params=pltpu.CompilerParams(vmem_limit_bytes=60 << 20),
        cost_estimate=pl.CostEstimate(
            flops=20 << 30, bytes_accessed=12 << 20, transcendentals=4 << 20
        ),
        name="attend",
    )(block_order, segment_ids[0].reshape(32, 128), q_own, q_sib, *w_ring, *k_ring, cs, *k_own, *k_sib)

    local_max = hm[:4, 0]
    low = jnp.full((4,), masked_value, f32)
    both = jnp.where(
        c == 0, jnp.concatenate([local_max, low]), jnp.concatenate([low, local_max])
    )
    head_max = of_everyone(both, ("seq", "dp"))
    ratio = CLIP / jnp.maximum(head_max, CLIP)
    root = jnp.sqrt(ratio)
    factors = jnp.concatenate(
        [jnp.broadcast_to(root[:, None], (8, NOPE)), jnp.broadcast_to(ratio[:, None], (8, ROPE))], axis=1
    ).reshape(8 * (NOPE + ROPE))
    clipped_uq = (w_uq.astype(f32) * factors[None, :]).astype(bf16)
    clipped_uk = (w_uk.astype(f32) * jnp.repeat(root, NOPE)[None, :]).astype(bf16)

    got = swap(ctx[256:])
    own = ctx[:256]
    first = c == 0
    context = jnp.concatenate([jnp.where(first, own, got), jnp.where(first, got, own)], axis=1)
    return (context[None], clipped_uq, clipped_uk)


def solution(mesh):
    placed = (
        P("dp", "seq", "tp"),
        P("dp", "seq", "tp"),
        P("dp", "seq", None),
        P("seq", "tp"),
        P("seq", "tp"),
        P("seq", "tp"),
        P("dp", None),
        P("dp", None),
    )
    return jax.shard_map(
        on_device,
        mesh=mesh,
        in_specs=placed,
        out_specs=(P("dp", "seq", "tp"), P("seq", "tp"), P("seq", "tp")),
        check_vma=False,
    )
```

```python
import math

import jax
import jax.numpy as jnp
from jax import lax
from jax.experimental import pallas as pl
from jax.experimental.pallas import tpu as pltpu
from jax.sharding import PartitionSpec as P


NOPE = 128
ROPE = 64
CLIP = 8
BLK = 128
CHUNK = 256

rope_base = 50000.0
masked_value = -1e30
scale = 1.0 / math.sqrt(NOPE + ROPE)

ANY = pl.BlockSpec(memory_space=pl.ANY)
SMEM = pl.BlockSpec(memory_space=pltpu.SMEM)
VMEM = pl.BlockSpec(memory_space=pltpu.VMEM)


def where_am_i():
    s, t = lax.axis_index("seq"), lax.axis_index("tp")
    return dict(z=s // 2, c=lax.rem(s, 2), y=lax.rem(t, 4), xl=t // 4)


def start_of(bounds, p):
    s = jnp.int32(0)
    for b in bounds:
        s = jnp.where(b <= p, jnp.maximum(s, b), s)
    return s


def feature_row(m, t, each):
    x, yy = t // 4, t % 4
    dy = lax.rem(yy - m["y"] + 4, 4)
    j = jnp.where(dy == 0, 0, jnp.where(dy == 1, 2, jnp.where(dy == 2, 3, 1)))
    xr = jnp.where(x == m["xl"], 0, 1)
    return (j * 2 + xr) * each


RING = [0, -1, 1, -2, 2, -3, 3, -4]


W_COLS = [[h * 192 + e * 32 for e in range(4)] for h in range(4)] + [
    [h * 192 + 128 for h in range(4)],
    [h * 192 + 160 for h in range(4)],
]


def split_kernel(q_t, k_t, w_uq, w_uk, w_uv, kq, w_mine, w_send, kv_mine, kv_send):
    c = where_am_i()["c"]
    kq[:64] = k_t[...]
    kq[64:] = q_t[...]

    def halves(own):
        for to, half in ((w_mine, own), (w_send, 1 - own)):
            for n, cols in enumerate(W_COLS):
                base = half * 768
                if n < 4:
                    block = w_uq[:, base + cols[0] : base + cols[0] + 128]
                else:
                    block = jnp.concatenate([w_uq[:, base + k : base + k + 32] for k in cols], axis=1)
                for b in range(3):
                    to[n * 3 + b] = block[b * 32 : (b + 1) * 32]
        for to, half in ((kv_mine, own), (kv_send, 1 - own)):
            for n in range(4):
                cols = slice(half * 512 + n * 128, half * 512 + n * 128 + 128)
                to[n] = w_uk[:, cols]
                to[4 + n] = w_uv[:, cols]

    @pl.when(c == 0)
    def _():
        halves(0)

    @pl.when(c == 1)
    def _():
        halves(1)


def turn_kernel(order, rope_t, cs, share, fold):
    m = where_am_i()
    pos = []
    lane = lax.broadcasted_iota(jnp.int32, (32, BLK), 1)
    for i in range(4):
        core = m["c"] if i < 2 else 1 - m["c"]
        pos.append(lane + order[0, (m["z"] * 2 + core) * 2 + i % 2] * BLK)
    steps = lax.broadcasted_iota(jnp.int32, (32, 512), 0).astype(jnp.float32) * (2.0 / ROPE)
    freqs = jnp.exp(-math.log(rope_base) * steps)
    angle = jnp.concatenate(pos, axis=1).astype(jnp.float32) * freqs
    cos, sin = jnp.cos(angle), jnp.sin(angle)
    cs[...] = jnp.concatenate([cos] * 4 + [sin] * 4, axis=0).T
    r = rope_t[...].astype(jnp.float32)
    a, b, rc, rs = r[:32], r[32:], cos[:, :256], sin[:, :256]
    both = jnp.concatenate([a * rc - b * rs, b * rc + a * rs], axis=0)
    fold[...] = jnp.concatenate([both[:, :128], both[:, 128:]], axis=0).T.astype(jnp.bfloat16)
    share[...] = fold[pl.ds(pl.multiple_of(m["y"] * 32, 32), 32), :]


def pack_kernel(kq, kq_x, share, w_mine, w_other, kv_mine, kv_other, k_one, w_one, q_x):
    c = where_am_i()["c"]
    lat = jnp.concatenate([kq[:64], kq_x[:64]], axis=0).T
    for b in range(8):
        k_one[b] = lat[b * 32 : (b + 1) * 32]
    k_one[8] = share[...]
    for core, w, kv in ((c, w_mine, kv_mine), (1 - c, w_other, kv_other)):
        for n in range(6):
            w_one[pl.ds(n * 6 + core * 3, 3)] = w[n * 3 : n * 3 + 3]
        for n in range(8):
            w_one[36 + n * 2 + core] = kv[n]
    q_x[...] = jnp.concatenate([kq[64:], kq_x[64:]], axis=0).T


def join_kernel(*refs):
    ins, out, sem = refs[:8], refs[8], refs[9]
    copies = [pltpu.make_async_copy(r, out.at[j], sem.at[j]) for j, r in enumerate(ins)]
    for cp in copies:
        cp.start()
    for cp in copies:
        cp.wait()


def label_of(bounds, p):
    label = jnp.zeros_like(p)
    for b in bounds:
        label = label + jnp.where(p >= b, 1, 0)
    return label


SLOTS = 38
EMPTY = 37
to_exp2 = scale * math.log2(math.e)


def attend_kernel(order, seg, *refs):
    q_in, w_in, cs, pieces = refs[:2], refs[2:10], refs[10], (refs[11:16], refs[16:21])
    out, hm = refs[21:23]
    q, wp, w, kvw, lat, rope, kn, v, kr, qs, sbuf, mx, rm, acc, total, step_i, step_ch, need = refs[23:41]
    qsem, wsem, ksem = refs[41:]
    m = where_am_i()

    def block_of(i):
        core = jnp.where(i // 2 == 0, m["c"], 1 - m["c"])
        return order[0, (m["z"] * 2 + core) * 2 + lax.rem(i, 2)]

    f32, bf16 = jnp.float32, jnp.bfloat16
    first, second = [], []
    for half in range(2):
        first.append(pltpu.make_async_copy(q_in[half], q.at[half], qsem.at[half]))
    for j in range(8):
        first.append(pltpu.make_async_copy(w_in[j], wp.at[j], wsem.at[j]))
    for core in range(2):
        own, up, dn, f1, f2 = pieces[core]
        for n, (src, plane, start, count, dy) in enumerate(
            ((own, 0, 0, 8, 0), (up, 1, 0, 8, 3), (dn, 2, 0, 8, 1), (f1, 3, 0, 4, 2), (f2, 3, 4, 4, 2))
        ):
            rows = pl.ds(core * 8 + start, count)
            yq = pl.multiple_of(lax.rem(m["y"] + dy, 4) * 32, 32)
            second.append(
                pltpu.make_async_copy(src.at[:, :8], lat.at[plane, rows], ksem.at[core, n, 0])
            )
            second.append(
                pltpu.make_async_copy(
                    src.at[:, 8], rope.at[rows, pl.ds(yq, 32), :], ksem.at[core, n, 1]
                )
            )
    for cp in first + second:
        cp.start()

    bounds = [jnp.sum(jnp.where(seg[...] < l, 1, 0)) for l in (1, 2, 3)]

    for n in range(16):
        need[n] = 0
    count = jnp.int32(0)
    for i in range(4):
        pb = block_of(i)
        lo = start_of(bounds, pb * BLK) // CHUNK
        hi = pb // 2
        need[hi] = 1

        def add(ch, g, i=i):
            step_i[g] = i
            step_ch[g] = ch
            need[ch] = 1
            return g + 1

        count = lax.fori_loop(lo, hi, add, count)
    step_i[count] = 3
    step_ch[count] = block_of(3) // 2
    odd = lax.rem(count, 2)

    for cp in first:
        cp.wait()
    for j in range(8):
        t = lax.rem(m["z"] + RING[j] + 8, 8)
        row = pl.multiple_of(feature_row(m, t, 192), 64)
        for n in range(6):
            w[pl.ds(row, 192), n * 128 : (n + 1) * 128] = wp[j, n * 6 : n * 6 + 6].reshape(192, 128)
        row = pl.multiple_of(feature_row(m, t, 64), 64)
        for n in range(8):
            kvw[pl.ds(row, 64), n * 128 : (n + 1) * 128] = wp[j, 36 + n * 2 : 38 + n * 2].reshape(64, 128)

    lane = lax.broadcasted_iota(jnp.int32, (BLK, 128), 1)
    line = lax.broadcasted_iota(jnp.int32, (BLK, 128), 0)
    for half in range(2):
        full = jnp.dot(q[half], w[...], preferred_element_type=f32)
        for b in range(2):
            part = slice(b * BLK, (b + 1) * BLK)
            rows = slice(half * 256 + b * BLK, half * 256 + (b + 1) * BLK)
            label = label_of(bounds, line + block_of(half * 2 + b) * BLK)
            onehot = jnp.where(lane == label + 64, 1.0, 0.0)
            cos, sin = cs[rows, :128], cs[rows, 128:]
            x, y = full[part, 512:640], full[part, 640:]
            rot = (x * cos - y * sin, y * cos + x * sin)
            for h in range(4):
                r0 = pltpu.roll(rot[0], (128 - 32 * h) % 128, 1) if h else rot[0]
                r1 = pltpu.roll(rot[1], (32 - 32 * h) % 128, 1) if h != 1 else rot[1]
                tail = jnp.where(lane < 32, r0, jnp.where(lane < 64, r1, onehot))
                qs[h, rows, :128] = full[part, h * 128 : (h + 1) * 128].astype(bf16)
                qs[h, rows, 128:] = tail.astype(bf16)

    mx[...] = jnp.full(mx.shape, masked_value, f32)
    acc[...] = jnp.zeros(acc.shape, f32)
    total[...] = jnp.zeros(total.shape, f32)
    sbuf[EMPTY] = jnp.full((4, BLK, CHUNK), masked_value, f32)
    for cp in second:
        cp.wait()

    def project(i, carry):
        j = lax.rem(i, 8)
        s = (j + 1) // 2
        dz = jnp.where(lax.rem(j, 2) == 1, -s, s)
        zz = lax.rem(m["z"] + dz + 8, 8)
        cc = jnp.where(i < 8, m["c"], 1 - m["c"])
        base = (zz * 2 + cc) * 2

        @pl.when((need[order[0, base] // 2] + need[order[0, base + 1] // 2]) > 0)
        def _():
            x = jnp.concatenate([lat[n, i].reshape(256, 128) for n in range(4)], axis=1)
            y = jnp.dot(x, kvw[...], preferred_element_type=f32)
            fold = rope[i]
            for b in range(2):
                pb = pl.multiple_of(order[0, base + b] * BLK, BLK)
                rows = slice(b * BLK, (b + 1) * BLK)
                kn[pl.ds(pb, BLK), :] = y[rows, :512].astype(bf16)
                v[pl.ds(pb, BLK), :] = y[rows, 512:].astype(bf16)
                label = label_of(bounds, line[:, :64] + pb)
                apart = jnp.where((lane[:, :64] < 4) & (lane[:, :64] != label), masked_value, 0.0)
                kr[pl.ds(pb, BLK), :] = jnp.concatenate(
                    [fold[:, b * 64 : b * 64 + 64], apart.astype(bf16)], axis=1
                )

        return carry

    lax.fori_loop(0, 16, project, 0)

    def scores(i, ch):
        keys = pl.ds(pl.multiple_of(ch * CHUNK, CHUNK), CHUNK)
        rows = pl.ds(pl.multiple_of(i * BLK, BLK), BLK)
        got = []
        for h in range(4):
            k = jnp.concatenate([kn[keys, h * 128 : (h + 1) * 128], kr[keys, :]], axis=1)
            got.append(
                lax.dot_general(
                    qs[h, rows, :], k, (((1,), (1,)), ((), ())), preferred_element_type=f32
                )
            )
        return got

    def keep(i, slot, h, s):
        sbuf[slot, h] = s
        mx[i, h] = jnp.maximum(mx[i, h], jnp.maximum(s[:, :128], s[:, 128:]))

    def diagonal(i, carry):
        pb = block_of(i)
        ch = pb // 2
        row = lax.broadcasted_iota(jnp.int32, (BLK, CHUNK), 0) + (pb * BLK - ch * CHUNK)
        col = lax.broadcasted_iota(jnp.int32, (BLK, CHUNK), 1)
        bias = jnp.where(col <= row, 0.0, masked_value)
        for h, s in enumerate(scores(i, ch)):
            keep(i, i, h, s + bias)
        return carry

    lax.fori_loop(0, 4, diagonal, 0)

    def score_pair(n, carry):
        picks = []
        for g in (2 * n, jnp.minimum(2 * n + 1, count - 1)):
            i, ch = step_i[g], step_ch[g]
            picks.append((i, g + 4, scores(i, ch)))
        for i, slot, got in picks:
            for h, s in enumerate(got):
                keep(i, slot, h, s)
        return carry

    pairs = (count + odd) // 2
    lax.fori_loop(0, pairs, score_pair, 0)

    hm[...] = jnp.full(hm.shape, masked_value, f32)

    def finish_max(i, carry):
        for h in range(4):
            top = jnp.broadcast_to(jnp.max(mx[i, h], axis=1, keepdims=True), (BLK, 128))
            rm[i, h] = top * to_exp2
            best = jnp.max(top, axis=0, keepdims=True) * scale
            hm[h : h + 1, :] = jnp.maximum(hm[h : h + 1, :], best)
        return carry

    lax.fori_loop(0, 4, finish_max, 0)

    def mix(steps):
        for i, ch, slot in steps:
            keys = pl.ds(pl.multiple_of(ch * CHUNK, CHUNK), CHUNK)
            for h in range(4):
                s = sbuf[slot, h]
                top = rm[i, h]
                p0 = jnp.exp2(s[:, :128] * to_exp2 - top)
                p1 = jnp.exp2(s[:, 128:] * to_exp2 - top)
                total[i, h] += p0 + p1
                p = jnp.concatenate([p0, p1], axis=1).astype(bf16)
                acc[i, h] += jnp.dot(p, v[keys, h * 128 : (h + 1) * 128], preferred_element_type=f32)

    def mix_diagonal(n, carry):
        mix([(2 * n + e, block_of(2 * n + e) // 2, 2 * n + e) for e in range(2)])
        return carry

    lax.fori_loop(0, 2, mix_diagonal, 0)

    def mix_pair(n, carry):
        a, b = 2 * n, 2 * n + 1
        slot = jnp.where(b < count, b + 4, EMPTY)
        mix([(step_i[a], step_ch[a], a + 4), (step_i[b], step_ch[b], slot)])
        return carry

    lax.fori_loop(0, pairs, mix_pair, 0)

    def finish(i, carry):
        rows = pl.ds(pl.multiple_of(i * BLK, BLK), BLK)
        for h in range(4):
            whole = jnp.sum(total[i, h], axis=1, keepdims=True)
            out[rows, h * 128 : (h + 1) * 128] = (acc[i, h] / whole).astype(bf16)
        return carry

    lax.fori_loop(0, 4, finish, 0)


def shift_seq(by):
    return [(i, (i + 2 * by) % 16) for i in range(16)]


SWAP = [(i, i ^ 1) for i in range(16)]
XSWAP = [(i, i ^ 4) for i in range(8)]


def shift_y(by):
    return [(x * 4 + y, x * 4 + (y + by) % 4) for x in range(2) for y in range(4)]


def ring(x):
    up, dn, got = x, x, [x]
    for s in range(1, 5):
        up = lax.ppermute(up, "seq", shift_seq(1))
        got.append(up)
        if s < 4:
            dn = lax.ppermute(dn, "seq", shift_seq(-1))
            got.append(dn)
    return got


def swap(x):
    return lax.ppermute(x, "seq", SWAP)


def call(kernel, outs, args, specs=None, scratch=()):
    outs = [jax.ShapeDtypeStruct(shape, dtype) for shape, dtype in outs]
    size = sum(math.prod(o.shape) * o.dtype.itemsize for o in outs)
    return pl.pallas_call(
        kernel,
        out_shape=outs,
        in_specs=specs or [VMEM] * len(args),
        out_specs=[VMEM] * len(outs),
        scratch_shapes=list(scratch),
        cost_estimate=pl.CostEstimate(flops=1 << 20, bytes_accessed=2 * size, transcendentals=0),
    )(*args)


def on_device(query_latent, key_latent, rope_key, w_uq, w_uk, w_uv, block_order, segment_ids):
    bf16, f32 = jnp.bfloat16, jnp.float32
    c = where_am_i()["c"]
    kq, w_mine, w_send, kv_mine, kv_send = call(
        split_kernel,
        [((256, 256), bf16)] + [((18, 32, 128), bf16)] * 2 + [((8, 32, 128), bf16)] * 2,
        (query_latent[0].T, key_latent[0].T, w_uq, w_uk, w_uv),
    )
    kq_x = lax.ppermute(kq, "tp", XSWAP)
    w_other = swap(w_send)
    kv_other = swap(kv_send)
    cs, share = call(
        turn_kernel,
        [((512, 256), f32), ((32, 128), bf16)],
        (block_order, rope_key[0].T),
        specs=[SMEM, VMEM],
        scratch=[pltpu.VMEM((128, 128), bf16)],
    )
    k_one, w_one, q_x = call(
        pack_kernel,
        [((9, 32, 128), bf16), ((52, 32, 128), bf16), ((256, 384), bf16)],
        (kq, kq_x, share, w_mine, w_other, kv_mine, kv_other),
    )

    k_ring = ring(k_one)
    w_ring = ring(w_one)
    q_parts = [q_x] + [lax.ppermute(q_x, "tp", shift_y(by)) for by in (1, -1, 2)]
    q_own = jnp.concatenate(q_parts, axis=1)
    q_sib = swap(q_own)
    (k_all,) = call(
        join_kernel,
        [((8, 9, 32, 128), bf16)],
        k_ring,
        specs=[ANY] * 8,
        scratch=[pltpu.SemaphoreType.DMA((8,))],
    )
    k_up = lax.ppermute(k_all, "tp", shift_y(1))
    k_dn = lax.ppermute(k_all, "tp", shift_y(-1))
    k_f1 = lax.ppermute(k_up[:4], "tp", shift_y(1))
    k_f2 = lax.ppermute(k_dn[4:], "tp", shift_y(-1))
    k_own = [k_all, k_up, k_dn, k_f1, k_f2]
    k_sib = [swap(p) for p in k_own]

    vm = pltpu.VMEM
    ctx, hm = pl.pallas_call(
        attend_kernel,
        out_shape=[
            jax.ShapeDtypeStruct((512, 512), bf16),
            jax.ShapeDtypeStruct((8, 128), f32),
        ],
        in_specs=[SMEM, VMEM] + [ANY] * 10 + [VMEM] + [ANY] * 10,
        out_specs=[VMEM] * 2,
        scratch_shapes=[
            vm((2, 256, 1536), bf16),
            vm((8, 52, 32, 128), bf16),
            vm((1536, 768), bf16),
            vm((512, 1024), bf16),
            vm((4, 16, 8, 32, 128), bf16),
            vm((16, 128, 128), bf16),
            vm((4096, 512), bf16),
            vm((4096, 512), bf16),
            vm((4096, 128), bf16),
            vm((4, 512, 256), bf16),
            vm((SLOTS, 4, BLK, CHUNK), f32),
            vm((4, 4, BLK, 128), f32),
            vm((4, 4, BLK, 128), f32),
            vm((4, 4, BLK, 128), f32),
            vm((4, 4, BLK, 128), f32),
            pltpu.SMEM((40,), jnp.int32),
            pltpu.SMEM((40,), jnp.int32),
            pltpu.SMEM((16,), jnp.int32),
            pltpu.SemaphoreType.DMA((2,)),
            pltpu.SemaphoreType.DMA((8,)),
            pltpu.SemaphoreType.DMA((2, 5, 2)),
        ],
        compiler_params=pltpu.CompilerParams(vmem_limit_bytes=60 << 20),
        cost_estimate=pl.CostEstimate(
            flops=20 << 30, bytes_accessed=12 << 20, transcendentals=4 << 20
        ),
        name="attend",
    )(block_order, segment_ids[0].reshape(32, 128), q_own, q_sib, *w_ring, cs, *k_own, *k_sib)

    local_max = hm[:4, 0]
    low = jnp.full((4,), masked_value, f32)
    both = jnp.where(
        c == 0, jnp.concatenate([local_max, low]), jnp.concatenate([low, local_max])
    )
    everyone = jnp.broadcast_to(both, (32, 8))
    everyone = lax.all_to_all(everyone, ("seq", "dp"), split_axis=0, concat_axis=0, tiled=True)
    got = swap(ctx[256:])
    own = ctx[:256]
    first = c == 0
    context = jnp.concatenate([jnp.where(first, own, got), jnp.where(first, got, own)], axis=1)
    everyone, context = lax.optimization_barrier((everyone, context))
    head_max = jnp.max(everyone, axis=0)
    ratio = CLIP / jnp.maximum(head_max, CLIP)
    root = jnp.sqrt(ratio)
    factors = jnp.concatenate(
        [jnp.broadcast_to(root[:, None], (8, NOPE)), jnp.broadcast_to(ratio[:, None], (8, ROPE))], axis=1
    ).reshape(8 * (NOPE + ROPE))
    clipped_uq = (w_uq.astype(f32) * factors[None, :]).astype(bf16)
    clipped_uk = (w_uk.astype(f32) * jnp.repeat(root, NOPE)[None, :]).astype(bf16)

    return (context[None], clipped_uq, clipped_uk)


def solution(mesh):
    placed = (
        P("dp", "seq", "tp"),
        P("dp", "seq", "tp"),
        P("dp", "seq", None),
        P("seq", "tp"),
        P("seq", "tp"),
        P("seq", "tp"),
        P("dp", None),
        P("dp", None),
    )
    return jax.shard_map(
        on_device,
        mesh=mesh,
        in_specs=placed,
        out_specs=(P("dp", "seq", "tp"), P("seq", "tp"), P("seq", "tp")),
        check_vma=False,
    )
```

```python
import math

import jax
import jax.numpy as jnp
from jax import lax
from jax.experimental import pallas as pl
from jax.experimental.pallas import tpu as pltpu
from jax.sharding import PartitionSpec as P


NOPE = 128
ROPE = 64
CLIP = 8
BLK = 128
CHUNK = 256

rope_base = 50000.0
masked_value = -1e30
scale = 1.0 / math.sqrt(NOPE + ROPE)

ANY = pl.BlockSpec(memory_space=pl.ANY)
SMEM = pl.BlockSpec(memory_space=pltpu.SMEM)
VMEM = pl.BlockSpec(memory_space=pltpu.VMEM)


def where_am_i():
    s, t = lax.axis_index("seq"), lax.axis_index("tp")
    return dict(z=s // 2, c=lax.rem(s, 2), y=lax.rem(t, 4), xl=t // 4)


def start_of(bounds, p):
    s = jnp.int32(0)
    for b in bounds:
        s = jnp.where(b <= p, jnp.maximum(s, b), s)
    return s


def feature_row(m, t, each):
    x, yy = t // 4, t % 4
    dy = lax.rem(yy - m["y"] + 4, 4)
    j = jnp.where(dy == 0, 0, jnp.where(dy == 1, 2, jnp.where(dy == 2, 3, 1)))
    xr = jnp.where(x == m["xl"], 0, 1)
    return (j * 2 + xr) * each


RING = [0, -1, 1, -2, 2, -3, 3, -4]


W_COLS = [[h * 192 + e * 32 for e in range(4)] for h in range(4)] + [
    [h * 192 + 128 for h in range(4)],
    [h * 192 + 160 for h in range(4)],
]


def split_kernel(q_t, k_t, w_uq, w_uk, w_uv, kq, w_mine, w_send, kv_mine, kv_send):
    c = where_am_i()["c"]
    kq[:64] = k_t[...]
    kq[64:] = q_t[...]

    def halves(own):
        for to, half in ((w_mine, own), (w_send, 1 - own)):
            for n, cols in enumerate(W_COLS):
                base = half * 768
                if n < 4:
                    block = w_uq[:, base + cols[0] : base + cols[0] + 128]
                else:
                    block = jnp.concatenate([w_uq[:, base + k : base + k + 32] for k in cols], axis=1)
                for b in range(3):
                    to[n * 3 + b] = block[b * 32 : (b + 1) * 32]
        for to, half in ((kv_mine, own), (kv_send, 1 - own)):
            for n in range(4):
                cols = slice(half * 512 + n * 128, half * 512 + n * 128 + 128)
                to[n] = w_uk[:, cols]
                to[4 + n] = w_uv[:, cols]

    @pl.when(c == 0)
    def _():
        halves(0)

    @pl.when(c == 1)
    def _():
        halves(1)


def turn_kernel(order, rope_t, cs, share, fold):
    m = where_am_i()
    pos = []
    lane = lax.broadcasted_iota(jnp.int32, (32, BLK), 1)
    for i in range(4):
        core = m["c"] if i < 2 else 1 - m["c"]
        pos.append(lane + order[0, (m["z"] * 2 + core) * 2 + i % 2] * BLK)
    steps = lax.broadcasted_iota(jnp.int32, (32, 512), 0).astype(jnp.float32) * (2.0 / ROPE)
    freqs = jnp.exp(-math.log(rope_base) * steps)
    angle = jnp.concatenate(pos, axis=1).astype(jnp.float32) * freqs
    cos, sin = jnp.cos(angle), jnp.sin(angle)
    cs[...] = jnp.concatenate([cos] * 4 + [sin] * 4, axis=0).T
    r = rope_t[...].astype(jnp.float32)
    a, b, rc, rs = r[:32], r[32:], cos[:, :256], sin[:, :256]
    both = jnp.concatenate([a * rc - b * rs, b * rc + a * rs], axis=0)
    fold[...] = jnp.concatenate([both[:, :128], both[:, 128:]], axis=0).T.astype(jnp.bfloat16)
    share[...] = fold[pl.ds(pl.multiple_of(m["y"] * 32, 32), 32), :]


def pack_kernel(kq, kq_x, share, w_mine, w_other, kv_mine, kv_other, k_one, w_one, q_x):
    c = where_am_i()["c"]
    lat = jnp.concatenate([kq[:64], kq_x[:64]], axis=0).T
    for b in range(8):
        k_one[b] = lat[b * 32 : (b + 1) * 32]
    k_one[8] = share[...]
    for core, w, kv in ((c, w_mine, kv_mine), (1 - c, w_other, kv_other)):
        for n in range(6):
            w_one[pl.ds(n * 6 + core * 3, 3)] = w[n * 3 : n * 3 + 3]
        for n in range(8):
            w_one[36 + n * 2 + core] = kv[n]
    q_x[...] = jnp.concatenate([kq[64:], kq_x[64:]], axis=0).T


def join_kernel(*refs):
    ins, out, sem = refs[:8], refs[8], refs[9]
    copies = [pltpu.make_async_copy(r, out.at[j], sem.at[j]) for j, r in enumerate(ins)]
    for cp in copies:
        cp.start()
    for cp in copies:
        cp.wait()


def clip_kernel(everyone, w_uq, w_uk, clipped_uq, clipped_uk):
    head_max = everyone[0]
    for n in range(1, 32):
        head_max = jnp.maximum(head_max, everyone[n])
    ratio = CLIP / jnp.maximum(head_max, CLIP)
    root = jnp.sqrt(ratio)
    for out, w, width in ((clipped_uq, w_uq, NOPE + ROPE), (clipped_uk, w_uk, NOPE)):
        lane = lax.broadcasted_iota(jnp.int32, (1, 8 * width), 1)
        factor = jnp.ones((1, 8 * width), jnp.float32)
        for h in range(8):
            here = jnp.where(lane < h * width + NOPE, root[:, h : h + 1], ratio[:, h : h + 1])
            factor = jnp.where(lane >= h * width, here, factor)
        out[...] = (w[...].astype(jnp.float32) * factor).astype(jnp.bfloat16)


def label_of(bounds, p):
    label = jnp.zeros_like(p)
    for b in bounds:
        label = label + jnp.where(p >= b, 1, 0)
    return label


SLOTS = 38
EMPTY = 37
to_exp2 = scale * math.log2(math.e)


def attend_kernel(order, seg, *refs):
    q_in, w_in, cs, pieces = refs[:2], refs[2:10], refs[10], (refs[11:16], refs[16:21])
    out, out_send, hm_out = refs[21:24]
    hm, q, wp, w, kvw, lat, rope, kn, v, kr, qs, sbuf, mx, rm, acc, total, step_i, step_ch, need = refs[24:43]
    qsem, wsem, ksem = refs[43:]
    m = where_am_i()

    def block_of(i):
        core = jnp.where(i // 2 == 0, m["c"], 1 - m["c"])
        return order[0, (m["z"] * 2 + core) * 2 + lax.rem(i, 2)]

    f32, bf16 = jnp.float32, jnp.bfloat16
    first, second = [], []
    for half in range(2):
        first.append(pltpu.make_async_copy(q_in[half], q.at[half], qsem.at[half]))
    for j in range(8):
        first.append(pltpu.make_async_copy(w_in[j], wp.at[j], wsem.at[j]))
    for core in range(2):
        own, up, dn, f1, f2 = pieces[core]
        for n, (src, plane, start, count, dy) in enumerate(
            ((own, 0, 0, 8, 0), (up, 1, 0, 8, 3), (dn, 2, 0, 8, 1), (f1, 3, 0, 4, 2), (f2, 3, 4, 4, 2))
        ):
            rows = pl.ds(core * 8 + start, count)
            yq = pl.multiple_of(lax.rem(m["y"] + dy, 4) * 32, 32)
            second.append(
                pltpu.make_async_copy(src.at[:, :8], lat.at[plane, rows], ksem.at[core, n, 0])
            )
            second.append(
                pltpu.make_async_copy(
                    src.at[:, 8], rope.at[rows, pl.ds(yq, 32), :], ksem.at[core, n, 1]
                )
            )
    for cp in first + second:
        cp.start()

    bounds = [jnp.sum(jnp.where(seg[...] < l, 1, 0)) for l in (1, 2, 3)]

    for n in range(16):
        need[n] = 0
    count = jnp.int32(0)
    for i in range(4):
        pb = block_of(i)
        lo = start_of(bounds, pb * BLK) // CHUNK
        hi = pb // 2
        need[hi] = 1

        def add(ch, g, i=i):
            step_i[g] = i
            step_ch[g] = ch
            need[ch] = 1
            return g + 1

        count = lax.fori_loop(lo, hi, add, count)
    step_i[count] = 3
    step_ch[count] = block_of(3) // 2
    odd = lax.rem(count, 2)

    for cp in first:
        cp.wait()
    for j in range(8):
        t = lax.rem(m["z"] + RING[j] + 8, 8)
        row = pl.multiple_of(feature_row(m, t, 192), 64)
        for n in range(6):
            w[pl.ds(row, 192), n * 128 : (n + 1) * 128] = wp[j, n * 6 : n * 6 + 6].reshape(192, 128)
        row = pl.multiple_of(feature_row(m, t, 64), 64)
        for n in range(8):
            kvw[pl.ds(row, 64), n * 128 : (n + 1) * 128] = wp[j, 36 + n * 2 : 38 + n * 2].reshape(64, 128)

    lane = lax.broadcasted_iota(jnp.int32, (BLK, 128), 1)
    line = lax.broadcasted_iota(jnp.int32, (BLK, 128), 0)
    for half in range(2):
        full = jnp.dot(q[half], w[...], preferred_element_type=f32)
        for b in range(2):
            part = slice(b * BLK, (b + 1) * BLK)
            rows = slice(half * 256 + b * BLK, half * 256 + (b + 1) * BLK)
            label = label_of(bounds, line + block_of(half * 2 + b) * BLK)
            onehot = jnp.where(lane == label + 64, 1.0, 0.0)
            cos, sin = cs[rows, :128], cs[rows, 128:]
            x, y = full[part, 512:640], full[part, 640:]
            rot = (x * cos - y * sin, y * cos + x * sin)
            for h in range(4):
                r0 = pltpu.roll(rot[0], (128 - 32 * h) % 128, 1) if h else rot[0]
                r1 = pltpu.roll(rot[1], (32 - 32 * h) % 128, 1) if h != 1 else rot[1]
                tail = jnp.where(lane < 32, r0, jnp.where(lane < 64, r1, onehot))
                qs[h, rows, :128] = full[part, h * 128 : (h + 1) * 128].astype(bf16)
                qs[h, rows, 128:] = tail.astype(bf16)

    mx[...] = jnp.full(mx.shape, masked_value, f32)
    acc[...] = jnp.zeros(acc.shape, f32)
    total[...] = jnp.zeros(total.shape, f32)
    sbuf[EMPTY] = jnp.full((4, BLK, CHUNK), masked_value, f32)
    for cp in second:
        cp.wait()

    def project(i, carry):
        j = lax.rem(i, 8)
        s = (j + 1) // 2
        dz = jnp.where(lax.rem(j, 2) == 1, -s, s)
        zz = lax.rem(m["z"] + dz + 8, 8)
        cc = jnp.where(i < 8, m["c"], 1 - m["c"])
        base = (zz * 2 + cc) * 2

        @pl.when((need[order[0, base] // 2] + need[order[0, base + 1] // 2]) > 0)
        def _():
            x = jnp.concatenate([lat[n, i].reshape(256, 128) for n in range(4)], axis=1)
            y = jnp.dot(x, kvw[...], preferred_element_type=f32)
            fold = rope[i]
            for b in range(2):
                pb = pl.multiple_of(order[0, base + b] * BLK, BLK)
                rows = slice(b * BLK, (b + 1) * BLK)
                kn[pl.ds(pb, BLK), :] = y[rows, :512].astype(bf16)
                v[pl.ds(pb, BLK), :] = y[rows, 512:].astype(bf16)
                label = label_of(bounds, line[:, :64] + pb)
                apart = jnp.where((lane[:, :64] < 4) & (lane[:, :64] != label), masked_value, 0.0)
                kr[pl.ds(pb, BLK), :] = jnp.concatenate(
                    [fold[:, b * 64 : b * 64 + 64], apart.astype(bf16)], axis=1
                )

        return carry

    lax.fori_loop(0, 16, project, 0)

    def scores(i, ch):
        keys = pl.ds(pl.multiple_of(ch * CHUNK, CHUNK), CHUNK)
        rows = pl.ds(pl.multiple_of(i * BLK, BLK), BLK)
        got = []
        for h in range(4):
            k = jnp.concatenate([kn[keys, h * 128 : (h + 1) * 128], kr[keys, :]], axis=1)
            got.append(
                lax.dot_general(
                    qs[h, rows, :], k, (((1,), (1,)), ((), ())), preferred_element_type=f32
                )
            )
        return got

    def keep(i, slot, h, s):
        sbuf[slot, h] = s
        mx[i, h] = jnp.maximum(mx[i, h], jnp.maximum(s[:, :128], s[:, 128:]))

    def diagonal(i, carry):
        pb = block_of(i)
        ch = pb // 2
        row = lax.broadcasted_iota(jnp.int32, (BLK, CHUNK), 0) + (pb * BLK - ch * CHUNK)
        col = lax.broadcasted_iota(jnp.int32, (BLK, CHUNK), 1)
        bias = jnp.where(col <= row, 0.0, masked_value)
        for h, s in enumerate(scores(i, ch)):
            keep(i, i, h, s + bias)
        return carry

    lax.fori_loop(0, 4, diagonal, 0)

    def score_pair(n, carry):
        picks = []
        for g in (2 * n, jnp.minimum(2 * n + 1, count - 1)):
            i, ch = step_i[g], step_ch[g]
            picks.append((i, g + 4, scores(i, ch)))
        for i, slot, got in picks:
            for h, s in enumerate(got):
                keep(i, slot, h, s)
        return carry

    pairs = (count + odd) // 2
    lax.fori_loop(0, pairs, score_pair, 0)

    hm[...] = jnp.full(hm.shape, masked_value, f32)

    def finish_max(i, carry):
        for h in range(4):
            top = jnp.broadcast_to(jnp.max(mx[i, h], axis=1, keepdims=True), (BLK, 128))
            rm[i, h] = top * to_exp2
            best = jnp.max(top, axis=0, keepdims=True) * scale
            best = jnp.where(lane[:1] == m["c"] * 4 + h, best, masked_value)
            hm[:1, :] = jnp.maximum(hm[:1, :], best)
        return carry

    lax.fori_loop(0, 4, finish_max, 0)
    hm_out[...] = jnp.broadcast_to(hm[:1, :8].reshape(1, 1, 8), (32, 1, 8))

    def mix(steps):
        for i, ch, slot in steps:
            keys = pl.ds(pl.multiple_of(ch * CHUNK, CHUNK), CHUNK)
            for h in range(4):
                s = sbuf[slot, h]
                top = rm[i, h]
                p0 = jnp.exp2(s[:, :128] * to_exp2 - top)
                p1 = jnp.exp2(s[:, 128:] * to_exp2 - top)
                total[i, h] += p0 + p1
                p = jnp.concatenate([p0, p1], axis=1).astype(bf16)
                acc[i, h] += jnp.dot(p, v[keys, h * 128 : (h + 1) * 128], preferred_element_type=f32)

    def mix_diagonal(n, carry):
        mix([(2 * n + e, block_of(2 * n + e) // 2, 2 * n + e) for e in range(2)])
        return carry

    lax.fori_loop(0, 2, mix_diagonal, 0)

    def mix_pair(n, carry):
        a, b = 2 * n, 2 * n + 1
        slot = jnp.where(b < count, b + 4, EMPTY)
        mix([(step_i[a], step_ch[a], a + 4), (step_i[b], step_ch[b], slot)])
        return carry

    lax.fori_loop(0, pairs, mix_pair, 0)

    for to, first_block in ((out, 0), (out_send, 2)):

        def finish(i, carry, to=to, first_block=first_block):
            rows = pl.ds(pl.multiple_of(i * BLK, BLK), BLK)
            for h in range(4):
                whole = jnp.sum(total[i + first_block, h], axis=1, keepdims=True)
                to[rows, h * 128 : (h + 1) * 128] = (acc[i + first_block, h] / whole).astype(bf16)
            return carry

        lax.fori_loop(0, 2, finish, 0)


def shift_seq(by):
    return [(i, (i + 2 * by) % 16) for i in range(16)]


SWAP = [(i, i ^ 1) for i in range(16)]
XSWAP = [(i, i ^ 4) for i in range(8)]


def shift_y(by):
    return [(x * 4 + y, x * 4 + (y + by) % 4) for x in range(2) for y in range(4)]


def ring(x):
    up, dn, got = x, x, [x]
    for s in range(1, 5):
        up = lax.ppermute(up, "seq", shift_seq(1))
        got.append(up)
        if s < 4:
            dn = lax.ppermute(dn, "seq", shift_seq(-1))
            got.append(dn)
    return got


def swap(x):
    return lax.ppermute(x, "seq", SWAP)


def call(kernel, outs, args, specs=None, scratch=()):
    outs = [jax.ShapeDtypeStruct(shape, dtype) for shape, dtype in outs]
    size = sum(math.prod(o.shape) * o.dtype.itemsize for o in outs)
    return pl.pallas_call(
        kernel,
        out_shape=outs,
        in_specs=specs or [VMEM] * len(args),
        out_specs=[VMEM] * len(outs),
        scratch_shapes=list(scratch),
        cost_estimate=pl.CostEstimate(flops=1 << 20, bytes_accessed=2 * size, transcendentals=0),
    )(*args)


def on_device(query_latent, key_latent, rope_key, w_uq, w_uk, w_uv, block_order, segment_ids):
    bf16, f32 = jnp.bfloat16, jnp.float32
    c = where_am_i()["c"]
    kq, w_mine, w_send, kv_mine, kv_send = call(
        split_kernel,
        [((256, 256), bf16)] + [((18, 32, 128), bf16)] * 2 + [((8, 32, 128), bf16)] * 2,
        (query_latent[0].T, key_latent[0].T, w_uq, w_uk, w_uv),
    )
    kq_x = lax.ppermute(kq, "tp", XSWAP)
    w_other = swap(w_send)
    kv_other = swap(kv_send)
    cs, share = call(
        turn_kernel,
        [((512, 256), f32), ((32, 128), bf16)],
        (block_order, rope_key[0].T),
        specs=[SMEM, VMEM],
        scratch=[pltpu.VMEM((128, 128), bf16)],
    )
    k_one, w_one, q_x = call(
        pack_kernel,
        [((9, 32, 128), bf16), ((52, 32, 128), bf16), ((256, 384), bf16)],
        (kq, kq_x, share, w_mine, w_other, kv_mine, kv_other),
    )

    k_ring = ring(k_one)
    w_ring = ring(w_one)
    q_parts = [q_x] + [lax.ppermute(q_x, "tp", shift_y(by)) for by in (1, -1, 2)]
    q_own = jnp.concatenate(q_parts, axis=1)
    q_sib = swap(q_own)
    (k_all,) = call(
        join_kernel,
        [((8, 9, 32, 128), bf16)],
        k_ring,
        specs=[ANY] * 8,
        scratch=[pltpu.SemaphoreType.DMA((8,))],
    )
    k_up = lax.ppermute(k_all, "tp", shift_y(1))
    k_dn = lax.ppermute(k_all, "tp", shift_y(-1))
    k_f1 = lax.ppermute(k_up[:4], "tp", shift_y(1))
    k_f2 = lax.ppermute(k_dn[4:], "tp", shift_y(-1))
    k_own = [k_all, k_up, k_dn, k_f1, k_f2]
    k_sib = [swap(p) for p in k_own]

    vm = pltpu.VMEM
    ctx, ctx_send, everyone = pl.pallas_call(
        attend_kernel,
        out_shape=[
            jax.ShapeDtypeStruct((256, 512), bf16),
            jax.ShapeDtypeStruct((256, 512), bf16),
            jax.ShapeDtypeStruct((32, 1, 8), f32),
        ],
        in_specs=[SMEM, VMEM] + [ANY] * 10 + [VMEM] + [ANY] * 10,
        out_specs=[VMEM] * 3,
        scratch_shapes=[
            vm((8, 128), f32),
            vm((2, 256, 1536), bf16),
            vm((8, 52, 32, 128), bf16),
            vm((1536, 768), bf16),
            vm((512, 1024), bf16),
            vm((4, 16, 8, 32, 128), bf16),
            vm((16, 128, 128), bf16),
            vm((4096, 512), bf16),
            vm((4096, 512), bf16),
            vm((4096, 128), bf16),
            vm((4, 512, 256), bf16),
            vm((SLOTS, 4, BLK, CHUNK), f32),
            vm((4, 4, BLK, 128), f32),
            vm((4, 4, BLK, 128), f32),
            vm((4, 4, BLK, 128), f32),
            vm((4, 4, BLK, 128), f32),
            pltpu.SMEM((40,), jnp.int32),
            pltpu.SMEM((40,), jnp.int32),
            pltpu.SMEM((16,), jnp.int32),
            pltpu.SemaphoreType.DMA((2,)),
            pltpu.SemaphoreType.DMA((8,)),
            pltpu.SemaphoreType.DMA((2, 5, 2)),
        ],
        compiler_params=pltpu.CompilerParams(vmem_limit_bytes=60 << 20),
        cost_estimate=pl.CostEstimate(
            flops=20 << 30, bytes_accessed=12 << 20, transcendentals=4 << 20
        ),
        name="attend",
    )(block_order, segment_ids[0].reshape(32, 128), q_own, q_sib, *w_ring, cs, *k_own, *k_sib)

    everyone = lax.all_to_all(everyone, ("seq", "dp"), split_axis=0, concat_axis=0, tiled=True)
    got = swap(ctx_send)
    first = c == 0
    context = jnp.concatenate([jnp.where(first, ctx, got), jnp.where(first, got, ctx)], axis=1)
    everyone, context = lax.optimization_barrier((everyone, context))
    clipped_uq, clipped_uk = call(
        clip_kernel, [((96, 1536), bf16), ((32, 1024), bf16)], (everyone, w_uq, w_uk)
    )
    return (context[None], clipped_uq, clipped_uk)


def solution(mesh):
    placed = (
        P("dp", "seq", "tp"),
        P("dp", "seq", "tp"),
        P("dp", "seq", None),
        P("seq", "tp"),
        P("seq", "tp"),
        P("seq", "tp"),
        P("dp", None),
        P("dp", None),
    )
    return jax.shard_map(
        on_device,
        mesh=mesh,
        in_specs=placed,
        out_specs=(P("dp", "seq", "tp"), P("seq", "tp"), P("seq", "tp")),
        check_vma=False,
    )
```

```python
import math

import jax
import jax.numpy as jnp
from jax import lax
from jax.experimental import pallas as pl
from jax.experimental.pallas import tpu as pltpu
from jax.sharding import PartitionSpec as P


NOPE = 128
ROPE = 64
CLIP = 8
BLK = 128
CHUNK = 256

rope_base = 50000.0
masked_value = -1e30
scale = 1.0 / math.sqrt(NOPE + ROPE)

ANY = pl.BlockSpec(memory_space=pl.ANY)
SMEM = pl.BlockSpec(memory_space=pltpu.SMEM)
VMEM = pl.BlockSpec(memory_space=pltpu.VMEM)


def where_am_i():
    s, t = lax.axis_index("seq"), lax.axis_index("tp")
    return dict(z=s // 2, c=lax.rem(s, 2), y=lax.rem(t, 4), xl=t // 4)


def start_of(bounds, p):
    s = jnp.int32(0)
    for b in bounds:
        s = jnp.where(b <= p, jnp.maximum(s, b), s)
    return s


def feature_row(m, t, each):
    x, yy = t // 4, t % 4
    dy = lax.rem(yy - m["y"] + 4, 4)
    j = jnp.where(dy == 0, 0, jnp.where(dy == 1, 2, jnp.where(dy == 2, 3, 1)))
    xr = jnp.where(x == m["xl"], 0, 1)
    return (j * 2 + xr) * each


RING = [0, -1, 1, -2, 2, -3, 3, -4]


def ring_shift(j):
    return jnp.where(lax.rem(j, 2) == 1, -((j + 1) // 2), (j + 1) // 2)


W_COLS = [[h * 192 + e * 32 for e in range(4)] for h in range(4)] + [
    [h * 192 + 128 for h in range(4)],
    [h * 192 + 160 for h in range(4)],
]


def split_kernel(q_t, k_t, w_uq, w_uk, w_uv, kq, w_mine, w_send, kv_mine, kv_send):
    c = where_am_i()["c"]
    kq[:64] = k_t[...]
    kq[64:] = q_t[...]

    def halves(own):
        for to, half in ((w_mine, own), (w_send, 1 - own)):
            for n, cols in enumerate(W_COLS):
                base = half * 768
                if n < 4:
                    block = w_uq[:, base + cols[0] : base + cols[0] + 128]
                else:
                    block = jnp.concatenate([w_uq[:, base + k : base + k + 32] for k in cols], axis=1)
                for b in range(3):
                    to[n * 3 + b] = block[b * 32 : (b + 1) * 32]
        for to, half in ((kv_mine, own), (kv_send, 1 - own)):
            for n in range(4):
                cols = slice(half * 512 + n * 128, half * 512 + n * 128 + 128)
                to[n] = w_uk[:, cols]
                to[4 + n] = w_uv[:, cols]

    @pl.when(c == 0)
    def _():
        halves(0)

    @pl.when(c == 1)
    def _():
        halves(1)


def turn_kernel(order, rope_t, cs, share, fold):
    m = where_am_i()
    pos = []
    lane = lax.broadcasted_iota(jnp.int32, (32, BLK), 1)
    for i in range(4):
        core = m["c"] if i < 2 else 1 - m["c"]
        pos.append(lane + order[0, (m["z"] * 2 + core) * 2 + i % 2] * BLK)
    steps = lax.broadcasted_iota(jnp.int32, (32, 512), 0).astype(jnp.float32) * (2.0 / ROPE)
    freqs = jnp.exp(-math.log(rope_base) * steps)
    angle = jnp.concatenate(pos, axis=1).astype(jnp.float32) * freqs
    cos, sin = jnp.cos(angle), jnp.sin(angle)
    cs[...] = jnp.concatenate([cos] * 4 + [sin] * 4, axis=0).T
    r = rope_t[...].astype(jnp.float32)
    a, b, rc, rs = r[:32], r[32:], cos[:, :256], sin[:, :256]
    both = jnp.concatenate([a * rc - b * rs, b * rc + a * rs], axis=0)
    fold[...] = jnp.concatenate([both[:, :128], both[:, 128:]], axis=0).T.astype(jnp.bfloat16)
    share[...] = fold[pl.ds(pl.multiple_of(m["y"] * 32, 32), 32), :]


def pack_kernel(kq, kq_x, share, w_mine, w_other, kv_mine, kv_other, k_one, w_one, q_x):
    c = where_am_i()["c"]
    lat = jnp.concatenate([kq[:64], kq_x[:64]], axis=0).T
    for b in range(8):
        k_one[b] = lat[b * 32 : (b + 1) * 32]
    k_one[8] = share[...]
    for core, w, kv in ((c, w_mine, kv_mine), (1 - c, w_other, kv_other)):
        for n in range(6):
            w_one[pl.ds(n * 6 + core * 3, 3)] = w[n * 3 : n * 3 + 3]
        for n in range(8):
            w_one[36 + n * 2 + core] = kv[n]
    q_x[...] = jnp.concatenate([kq[64:], kq_x[64:]], axis=0).T


def join_kernel(*refs):
    ins, out, sem = refs[:8], refs[8], refs[9]
    copies = [pltpu.make_async_copy(r, out.at[j], sem.at[j]) for j, r in enumerate(ins)]
    for cp in copies:
        cp.start()
    for cp in copies:
        cp.wait()


def clip_kernel(everyone, w_uq, w_uk, clipped_uq, clipped_uk):
    head_max = everyone[0]
    for n in range(1, 32):
        head_max = jnp.maximum(head_max, everyone[n])
    ratio = CLIP / jnp.maximum(head_max, CLIP)
    root = jnp.sqrt(ratio)
    for out, w, width in ((clipped_uq, w_uq, NOPE + ROPE), (clipped_uk, w_uk, NOPE)):
        lane = lax.broadcasted_iota(jnp.int32, (1, 8 * width), 1)
        factor = jnp.ones((1, 8 * width), jnp.float32)
        for h in range(8):
            here = jnp.where(lane < h * width + NOPE, root[:, h : h + 1], ratio[:, h : h + 1])
            factor = jnp.where(lane >= h * width, here, factor)
        out[...] = (w[...].astype(jnp.float32) * factor).astype(jnp.bfloat16)


def label_of(bounds, p):
    label = jnp.zeros_like(p)
    for b in bounds:
        label = label + jnp.where(p >= b, 1, 0)
    return label


SLOTS = 38
EMPTY = 37
to_exp2 = scale * math.log2(math.e)


def attend_kernel(order, seg, *refs):
    q_in, w_in, refs = refs[:2], refs[2:11], refs[1:]
    cs, pieces = refs[10], (refs[11:16], refs[16:21])
    out, out_send, hm_out = refs[21:24]
    hm, q, wp, w, kvw, lat, rope, kn, v, kr, qs, sbuf, mx, rm, acc, total, step_i, step_ch, need, use = refs[24:44]
    qsem, wsem, ksem = refs[44:]
    m = where_am_i()

    def block_of(i):
        core = jnp.where(i // 2 == 0, m["c"], 1 - m["c"])
        return order[0, (m["z"] * 2 + core) * 2 + lax.rem(i, 2)]

    f32, bf16 = jnp.float32, jnp.bfloat16
    first, second = [], []
    for half in range(2):
        first.append(pltpu.make_async_copy(q_in[half], q.at[half], qsem.at[half]))
    for j in range(7):
        first.append(pltpu.make_async_copy(w_in[j], wp.at[j], wsem.at[j]))
    for e in range(2):
        first.append(pltpu.make_async_copy(w_in[7 + e], wp.at[7, pl.ds(26 * e, 26)], wsem.at[7 + e]))
    for core in range(2):
        own, up, dn, f1, f2 = pieces[core]
        for n, (src, plane, start, count, dy) in enumerate(
            ((own, 0, 0, 8, 0), (up, 1, 0, 8, 3), (dn, 2, 0, 8, 1), (f1, 3, 0, 4, 2), (f2, 3, 4, 4, 2))
        ):
            rows = pl.ds(core * 8 + start, count)
            yq = pl.multiple_of(lax.rem(m["y"] + dy, 4) * 32, 32)
            second.append(
                pltpu.make_async_copy(src.at[:, :8], lat.at[plane, rows], ksem.at[core, n, 0])
            )
            second.append(
                pltpu.make_async_copy(
                    src.at[:, 8], rope.at[rows, pl.ds(yq, 32), :], ksem.at[core, n, 1]
                )
            )
    for cp in first + second:
        cp.start()

    bounds = [jnp.sum(jnp.where(seg[...] < l, 1, 0)) for l in (1, 2, 3)]

    for n in range(16):
        need[n] = 0
    count = jnp.int32(0)
    for i in range(4):
        pb = block_of(i)
        lo = start_of(bounds, pb * BLK) // CHUNK
        hi = pb // 2
        need[hi] = 1

        def add(ch, g, i=i):
            step_i[g] = i
            step_ch[g] = ch
            need[ch] = 1
            return g + 1

        count = lax.fori_loop(lo, hi, add, count)
    step_i[count] = 3
    step_ch[count] = block_of(3) // 2

    for cp in first:
        cp.wait()
    for j in range(8):
        t = lax.rem(m["z"] + RING[j] + 8, 8)
        row = pl.multiple_of(feature_row(m, t, 192), 64)
        for n in range(6):
            w[pl.ds(row, 192), n * 128 : (n + 1) * 128] = wp[j, n * 6 : n * 6 + 6].reshape(192, 128)
        row = pl.multiple_of(feature_row(m, t, 64), 64)
        for n in range(8):
            kvw[pl.ds(row, 64), n * 128 : (n + 1) * 128] = wp[j, 36 + n * 2 : 38 + n * 2].reshape(64, 128)

    lane = lax.broadcasted_iota(jnp.int32, (BLK, 128), 1)
    line = lax.broadcasted_iota(jnp.int32, (BLK, 128), 0)
    for half in range(2):
        full = jnp.dot(q[half], w[...], preferred_element_type=f32)
        for b in range(2):
            part = slice(b * BLK, (b + 1) * BLK)
            rows = slice(half * 256 + b * BLK, half * 256 + (b + 1) * BLK)
            label = label_of(bounds, line + block_of(half * 2 + b) * BLK)
            onehot = jnp.where(lane == label + 64, 1.0, 0.0)
            cos, sin = cs[rows, :128], cs[rows, 128:]
            x, y = full[part, 512:640], full[part, 640:]
            rot = (x * cos - y * sin, y * cos + x * sin)
            for h in range(4):
                r0 = pltpu.roll(rot[0], (128 - 32 * h) % 128, 1) if h else rot[0]
                r1 = pltpu.roll(rot[1], (32 - 32 * h) % 128, 1) if h != 1 else rot[1]
                tail = jnp.where(lane < 32, r0, jnp.where(lane < 64, r1, onehot))
                qs[h, rows, :128] = full[part, h * 128 : (h + 1) * 128].astype(bf16)
                qs[h, rows, 128:] = tail.astype(bf16)

    mx[...] = jnp.full(mx.shape, masked_value, f32)
    acc[...] = jnp.zeros(acc.shape, f32)
    total[...] = jnp.zeros(total.shape, f32)
    sbuf[EMPTY] = jnp.full((4, BLK, CHUNK), masked_value, f32)
    for cp in second:
        cp.wait()

    def place(i):
        zz = lax.rem(m["z"] + ring_shift(lax.rem(i, 8)) + 8, 8)
        return (zz * 2 + jnp.where(i < 8, m["c"], 1 - m["c"])) * 2

    def pick(i, n):
        base = place(i)
        use[n] = i
        return n + jnp.minimum(need[order[0, base] // 2] + need[order[0, base + 1] // 2], 1)

    used = lax.fori_loop(0, 16, pick, jnp.int32(0))

    def project(n, carry):
        for i in (use[2 * n], use[jnp.minimum(2 * n + 1, used - 1)]):
            base = place(i)
            x = jnp.concatenate([lat[e, i].reshape(256, 128) for e in range(4)], axis=1)
            y = jnp.dot(x, kvw[...], preferred_element_type=f32)
            fold = rope[i]
            for b in range(2):
                pb = pl.multiple_of(order[0, base + b] * BLK, BLK)
                rows = slice(b * BLK, (b + 1) * BLK)
                kn[pl.ds(pb, BLK), :] = y[rows, :512].astype(bf16)
                v[pl.ds(pb, BLK), :] = y[rows, 512:].astype(bf16)
                label = label_of(bounds, line[:, :64] + pb)
                apart = jnp.where((lane[:, :64] < 4) & (lane[:, :64] != label), masked_value, 0.0)
                kr[pl.ds(pb, BLK), :] = jnp.concatenate(
                    [fold[:, b * 64 : b * 64 + 64], apart.astype(bf16)], axis=1
                )
        return carry

    lax.fori_loop(0, (used + 1) // 2, project, 0)

    def scores(i, ch):
        keys = pl.ds(pl.multiple_of(ch * CHUNK, CHUNK), CHUNK)
        rows = pl.ds(pl.multiple_of(i * BLK, BLK), BLK)
        got = []
        for h in range(4):
            k = jnp.concatenate([kn[keys, h * 128 : (h + 1) * 128], kr[keys, :]], axis=1)
            got.append(
                lax.dot_general(
                    qs[h, rows, :], k, (((1,), (1,)), ((), ())), preferred_element_type=f32
                )
            )
        return got

    def keep(i, slot, h, s):
        sbuf[slot, h] = s
        mx[i, h] = jnp.maximum(mx[i, h], jnp.maximum(s[:, :128], s[:, 128:]))

    def diagonal(i, carry):
        pb = block_of(i)
        ch = pb // 2
        row = lax.broadcasted_iota(jnp.int32, (BLK, CHUNK), 0) + (pb * BLK - ch * CHUNK)
        col = lax.broadcasted_iota(jnp.int32, (BLK, CHUNK), 1)
        bias = jnp.where(col <= row, 0.0, masked_value)
        for h, s in enumerate(scores(i, ch)):
            keep(i, i, h, s + bias)
        return carry

    lax.fori_loop(0, 4, diagonal, 0)

    def score_four(n, carry):
        picks = []
        for e in range(4):
            g = jnp.minimum(4 * n + e, count - 1)
            i, ch = step_i[g], step_ch[g]
            picks.append((i, g + 4, scores(i, ch)))
        for i, slot, got in picks:
            for h, s in enumerate(got):
                keep(i, slot, h, s)
        return carry

    fours = (count + 3) // 4
    lax.fori_loop(0, fours, score_four, 0)

    hm[...] = jnp.full(hm.shape, masked_value, f32)

    def finish_max(i, carry):
        for h in range(4):
            top = jnp.broadcast_to(jnp.max(mx[i, h], axis=1, keepdims=True), (BLK, 128))
            rm[i, h] = top * to_exp2
            best = jnp.max(top, axis=0, keepdims=True) * scale
            best = jnp.where(lane[:1] == m["c"] * 4 + h, best, masked_value)
            hm[:1, :] = jnp.maximum(hm[:1, :], best)
        return carry

    lax.fori_loop(0, 4, finish_max, 0)
    hm_out[...] = jnp.broadcast_to(hm[:1, :8].reshape(1, 1, 8), (32, 1, 8))

    def mix(steps):
        for i, ch, slot in steps:
            keys = pl.ds(pl.multiple_of(ch * CHUNK, CHUNK), CHUNK)
            for h in range(4):
                s = sbuf[slot, h]
                top = rm[i, h]
                p0 = jnp.exp2(s[:, :128] * to_exp2 - top)
                p1 = jnp.exp2(s[:, 128:] * to_exp2 - top)
                total[i, h] += p0 + p1
                p = jnp.concatenate([p0, p1], axis=1).astype(bf16)
                acc[i, h] += jnp.dot(p, v[keys, h * 128 : (h + 1) * 128], preferred_element_type=f32)

    def mix_diagonal(n, carry):
        mix([(2 * n + e, block_of(2 * n + e) // 2, 2 * n + e) for e in range(2)])
        return carry

    lax.fori_loop(0, 2, mix_diagonal, 0)

    def mix_four(n, carry):
        steps = []
        for e in range(4):
            g = 4 * n + e
            at = jnp.minimum(g, count)
            steps.append((step_i[at], step_ch[at], jnp.where(g < count, g + 4, EMPTY)))
        mix(steps)
        return carry

    lax.fori_loop(0, fours, mix_four, 0)

    for to, first_block in ((out, 0), (out_send, 2)):

        def finish(i, carry, to=to, first_block=first_block):
            rows = pl.ds(pl.multiple_of(i * BLK, BLK), BLK)
            for h in range(4):
                whole = jnp.sum(total[i + first_block, h], axis=1, keepdims=True)
                to[rows, h * 128 : (h + 1) * 128] = (acc[i + first_block, h] / whole).astype(bf16)
            return carry

        lax.fori_loop(0, 2, finish, 0)


def shift_seq(by):
    return [(i, (i + 2 * by) % 16) for i in range(16)]


SWAP = [(i, i ^ 1) for i in range(16)]
XSWAP = [(i, i ^ 4) for i in range(8)]


def shift_y(by):
    return [(x * 4 + y, x * 4 + (y + by) % 4) for x in range(2) for y in range(4)]


def move(x, axis, perm):
    return lax.ppermute(x, axis, perm)


def ring(x, last=4):
    up, dn, got = x, x, [x]
    for s in range(1, last + 1):
        up = move(up, "seq", shift_seq(1))
        got.append(up)
        if s < 4:
            dn = move(dn, "seq", shift_seq(-1))
            got.append(dn)
    return got


def swap(x):
    return move(x, "seq", SWAP)


def call(kernel, outs, args, specs=None, scratch=()):
    outs = [jax.ShapeDtypeStruct(shape, dtype) for shape, dtype in outs]
    size = sum(math.prod(o.shape) * o.dtype.itemsize for o in outs)
    return pl.pallas_call(
        kernel,
        out_shape=outs,
        in_specs=specs or [VMEM] * len(args),
        out_specs=[VMEM] * len(outs),
        scratch_shapes=list(scratch),
        cost_estimate=pl.CostEstimate(flops=1 << 20, bytes_accessed=2 * size, transcendentals=0),
    )(*args)


def on_device(query_latent, key_latent, rope_key, w_uq, w_uk, w_uv, block_order, segment_ids):
    bf16, f32 = jnp.bfloat16, jnp.float32
    c = where_am_i()["c"]
    kq, w_mine, w_send, kv_mine, kv_send = call(
        split_kernel,
        [((256, 256), bf16)] + [((18, 32, 128), bf16)] * 2 + [((8, 32, 128), bf16)] * 2,
        (query_latent[0].T, key_latent[0].T, w_uq, w_uk, w_uv),
    )
    kq_x = move(kq, "tp", XSWAP)
    w_other = swap(w_send)
    kv_other = swap(kv_send)
    cs, share = call(
        turn_kernel,
        [((512, 256), f32), ((32, 128), bf16)],
        (block_order, rope_key[0].T),
        specs=[SMEM, VMEM],
        scratch=[pltpu.VMEM((128, 128), bf16)],
    )
    k_one, w_one, q_x = call(
        pack_kernel,
        [((9, 32, 128), bf16), ((52, 32, 128), bf16), ((256, 384), bf16)],
        (kq, kq_x, share, w_mine, w_other, kv_mine, kv_other),
    )

    k_ring = ring(k_one)
    w_ring = ring(w_one, 3)
    w_ring += [move(w_ring[5][:26], "seq", shift_seq(1)), move(w_ring[6][26:], "seq", shift_seq(-1))]
    q_parts = [q_x] + [move(q_x, "tp", shift_y(by)) for by in (1, -1, 2)]
    q_own = jnp.concatenate(q_parts, axis=1)
    q_sib = swap(q_own)
    (k_all,) = call(
        join_kernel,
        [((8, 9, 32, 128), bf16)],
        k_ring,
        specs=[ANY] * 8,
        scratch=[pltpu.SemaphoreType.DMA((8,))],
    )
    k_up = move(k_all, "tp", shift_y(1))
    k_dn = move(k_all, "tp", shift_y(-1))
    k_f1 = move(k_up[:4], "tp", shift_y(1))
    k_f2 = move(k_dn[4:], "tp", shift_y(-1))
    k_own = [k_all, k_up, k_dn, k_f1, k_f2]
    k_sib = [swap(p) for p in k_own]

    vm = pltpu.VMEM
    ctx, ctx_send, everyone = pl.pallas_call(
        attend_kernel,
        out_shape=[
            jax.ShapeDtypeStruct((256, 512), bf16),
            jax.ShapeDtypeStruct((256, 512), bf16),
            jax.ShapeDtypeStruct((32, 1, 8), f32),
        ],
        in_specs=[SMEM, VMEM] + [ANY] * 11 + [VMEM] + [ANY] * 10,
        out_specs=[VMEM] * 3,
        scratch_shapes=[
            vm((8, 128), f32),
            vm((2, 256, 1536), bf16),
            vm((8, 52, 32, 128), bf16),
            vm((1536, 768), bf16),
            vm((512, 1024), bf16),
            vm((4, 16, 8, 32, 128), bf16),
            vm((16, 128, 128), bf16),
            vm((4096, 512), bf16),
            vm((4096, 512), bf16),
            vm((4096, 128), bf16),
            vm((4, 512, 256), bf16),
            vm((SLOTS, 4, BLK, CHUNK), f32),
            vm((4, 4, BLK, 128), f32),
            vm((4, 4, BLK, 128), f32),
            vm((4, 4, BLK, 128), f32),
            vm((4, 4, BLK, 128), f32),
            pltpu.SMEM((40,), jnp.int32),
            pltpu.SMEM((40,), jnp.int32),
            pltpu.SMEM((16,), jnp.int32),
            pltpu.SMEM((17,), jnp.int32),
            pltpu.SemaphoreType.DMA((2,)),
            pltpu.SemaphoreType.DMA((9,)),
            pltpu.SemaphoreType.DMA((2, 5, 2)),
        ],
        compiler_params=pltpu.CompilerParams(vmem_limit_bytes=60 << 20),
        cost_estimate=pl.CostEstimate(
            flops=20 << 30, bytes_accessed=12 << 20, transcendentals=4 << 20
        ),
        name="attend",
    )(block_order, segment_ids[0].reshape(32, 128), q_own, q_sib, *w_ring, cs, *k_own, *k_sib)

    everyone = lax.all_to_all(everyone, ("seq", "dp"), split_axis=0, concat_axis=0, tiled=True)
    got = swap(ctx_send)
    first = c == 0
    context = jnp.concatenate([jnp.where(first, ctx, got), jnp.where(first, got, ctx)], axis=1)
    everyone, context = lax.optimization_barrier((everyone, context))
    clipped_uq, clipped_uk = call(
        clip_kernel, [((96, 1536), bf16), ((32, 1024), bf16)], (everyone, w_uq, w_uk)
    )
    return (context[None], clipped_uq, clipped_uk)


def solution(mesh):
    placed = (
        P("dp", "seq", "tp"),
        P("dp", "seq", "tp"),
        P("dp", "seq", None),
        P("seq", "tp"),
        P("seq", "tp"),
        P("seq", "tp"),
        P("dp", None),
        P("dp", None),
    )
    return jax.shard_map(
        on_device,
        mesh=mesh,
        in_specs=placed,
        out_specs=(P("dp", "seq", "tp"), P("seq", "tp"), P("seq", "tp")),
        check_vma=False,
    )
```

```python
import math

import jax
import jax.numpy as jnp
from jax import lax
from jax.experimental import pallas as pl
from jax.experimental.pallas import tpu as pltpu
from jax.sharding import PartitionSpec as P


NOPE = 128
ROPE = 64
CLIP = 8
BLK = 128
CHUNK = 256

rope_base = 50000.0
masked_value = -1e30
scale = 1.0 / math.sqrt(NOPE + ROPE)

ANY = pl.BlockSpec(memory_space=pl.ANY)
SMEM = pl.BlockSpec(memory_space=pltpu.SMEM)
VMEM = pl.BlockSpec(memory_space=pltpu.VMEM)


def where_am_i():
    s, t = lax.axis_index("seq"), lax.axis_index("tp")
    return dict(z=s // 2, c=lax.rem(s, 2), y=lax.rem(t, 4), xl=t // 4)


def start_of(bounds, p):
    s = jnp.int32(0)
    for b in bounds:
        s = jnp.where(b <= p, jnp.maximum(s, b), s)
    return s


def feature_row(m, t, each):
    x, yy = t // 4, t % 4
    dy = lax.rem(yy - m["y"] + 4, 4)
    j = jnp.where(dy == 0, 0, jnp.where(dy == 1, 2, jnp.where(dy == 2, 3, 1)))
    xr = jnp.where(x == m["xl"], 0, 1)
    return (j * 2 + xr) * each


RING = [0, -1, 1, -2, 2, -3, 3, -4]


def ring_shift(j):
    return jnp.where(lax.rem(j, 2) == 1, -((j + 1) // 2), (j + 1) // 2)


W_COLS = [[h * 192 + e * 32 for e in range(4)] for h in range(4)] + [
    [h * 192 + 128 for h in range(4)],
    [h * 192 + 160 for h in range(4)],
]


def split_kernel(w_uq, w_uk, w_uv, w_mine, w_send, kv_mine, kv_send):
    c = where_am_i()["c"]

    def halves(own):
        for to, half in ((w_mine, own), (w_send, 1 - own)):
            for n, cols in enumerate(W_COLS):
                base = half * 768
                if n < 4:
                    block = w_uq[:, base + cols[0] : base + cols[0] + 128]
                else:
                    block = jnp.concatenate([w_uq[:, base + k : base + k + 32] for k in cols], axis=1)
                for b in range(3):
                    to[n * 3 + b] = block[b * 32 : (b + 1) * 32]
        for to, half in ((kv_mine, own), (kv_send, 1 - own)):
            for n in range(4):
                cols = slice(half * 512 + n * 128, half * 512 + n * 128 + 128)
                to[n] = w_uk[:, cols]
                to[4 + n] = w_uv[:, cols]

    @pl.when(c == 0)
    def _():
        halves(0)

    @pl.when(c == 1)
    def _():
        halves(1)


def turn_kernel(order, rope_t, cs, share, fold):
    m = where_am_i()
    pos = []
    lane = lax.broadcasted_iota(jnp.int32, (32, BLK), 1)
    for i in range(4):
        core = m["c"] if i < 2 else 1 - m["c"]
        pos.append(lane + order[0, (m["z"] * 2 + core) * 2 + i % 2] * BLK)
    steps = lax.broadcasted_iota(jnp.int32, (32, 512), 0).astype(jnp.float32) * (2.0 / ROPE)
    freqs = jnp.exp(-math.log(rope_base) * steps)
    angle = jnp.concatenate(pos, axis=1).astype(jnp.float32) * freqs
    cos, sin = jnp.cos(angle), jnp.sin(angle)
    cs[...] = jnp.concatenate([cos] * 4 + [sin] * 4, axis=0).T
    r = rope_t[...].astype(jnp.float32)
    a, b, rc, rs = r[:32], r[32:], cos[:, :256], sin[:, :256]
    both = jnp.concatenate([a * rc - b * rs, b * rc + a * rs], axis=0)
    fold[...] = jnp.concatenate([both[:, :128], both[:, 128:]], axis=0).T.astype(jnp.bfloat16)
    share[...] = fold[pl.ds(pl.multiple_of(m["y"] * 32, 32), 32), :]


def pack_kernel(k_t, k_tx, q_t, q_tx, share, w_mine, w_other, kv_mine, kv_other, k_one, w_one, q_x):
    c = where_am_i()["c"]
    lat = jnp.concatenate([k_t[...], k_tx[...]], axis=0).T
    for b in range(8):
        k_one[b] = lat[b * 32 : (b + 1) * 32]
    k_one[8] = share[...]
    for core, w, kv in ((c, w_mine, kv_mine), (1 - c, w_other, kv_other)):
        for n in range(6):
            w_one[pl.ds(n * 6 + core * 3, 3)] = w[n * 3 : n * 3 + 3]
        for n in range(8):
            w_one[36 + n * 2 + core] = kv[n]
    q_x[...] = jnp.concatenate([q_t[...], q_tx[...]], axis=0).T


def join_kernel(*refs):
    ins, out, sem = refs[:8], refs[8], refs[9]
    copies = [pltpu.make_async_copy(r, out.at[j], sem.at[j]) for j, r in enumerate(ins)]
    for cp in copies:
        cp.start()
    for cp in copies:
        cp.wait()


def clip_kernel(everyone, w_uq, w_uk, clipped_uq, clipped_uk):
    head_max = everyone[0]
    for n in range(1, 32):
        head_max = jnp.maximum(head_max, everyone[n])
    ratio = CLIP / jnp.maximum(head_max, CLIP)
    root = jnp.sqrt(ratio)
    for out, w, width in ((clipped_uq, w_uq, NOPE + ROPE), (clipped_uk, w_uk, NOPE)):
        lane = lax.broadcasted_iota(jnp.int32, (1, 8 * width), 1)
        factor = jnp.ones((1, 8 * width), jnp.float32)
        for h in range(8):
            here = jnp.where(lane < h * width + NOPE, root[:, h : h + 1], ratio[:, h : h + 1])
            factor = jnp.where(lane >= h * width, here, factor)
        out[...] = (w[...].astype(jnp.float32) * factor).astype(jnp.bfloat16)


def label_of(bounds, p):
    label = jnp.zeros_like(p)
    for b in bounds:
        label = label + jnp.where(p >= b, 1, 0)
    return label


SLOTS = 38
EMPTY = 37
to_exp2 = scale * math.log2(math.e)


def attend_kernel(order, seg, *refs):
    q_in, w_in, refs = refs[:2], refs[2:11], refs[1:]
    cs, pieces = refs[10], (refs[11:16], refs[16:21])
    out, out_send, hm_out = refs[21:24]
    hm, q, wp, w, kvw, lat, rope, kn, v, kr, qs, sbuf, mx, rm, acc, total, step_i, step_ch, need, use = refs[24:44]
    qsem, wsem, ksem = refs[44:]
    m = where_am_i()

    def block_of(i):
        core = jnp.where(i // 2 == 0, m["c"], 1 - m["c"])
        return order[0, (m["z"] * 2 + core) * 2 + lax.rem(i, 2)]

    f32, bf16 = jnp.float32, jnp.bfloat16
    first, second = [], []
    for half in range(2):
        first.append(pltpu.make_async_copy(q_in[half], q.at[half], qsem.at[half]))
    for j in range(7):
        first.append(pltpu.make_async_copy(w_in[j], wp.at[j], wsem.at[j]))
    for e in range(2):
        first.append(pltpu.make_async_copy(w_in[7 + e], wp.at[7, pl.ds(26 * e, 26)], wsem.at[7 + e]))
    for core in range(2):
        own, up, dn, f1, f2 = pieces[core]
        for n, (src, plane, start, count, dy) in enumerate(
            ((own, 0, 0, 8, 0), (up, 1, 0, 8, 3), (dn, 2, 0, 8, 1), (f1, 3, 0, 4, 2), (f2, 3, 4, 4, 2))
        ):
            rows = pl.ds(core * 8 + start, count)
            yq = pl.multiple_of(lax.rem(m["y"] + dy, 4) * 32, 32)
            second.append(
                pltpu.make_async_copy(src.at[:, :8], lat.at[plane, rows], ksem.at[core, n, 0])
            )
            second.append(
                pltpu.make_async_copy(
                    src.at[:, 8], rope.at[rows, pl.ds(yq, 32), :], ksem.at[core, n, 1]
                )
            )
    for cp in first + second:
        cp.start()

    bounds = [jnp.sum(jnp.where(seg[...] < l, 1, 0)) for l in (1, 2, 3)]

    for n in range(16):
        need[n] = 0
    count = jnp.int32(0)
    for i in range(4):
        pb = block_of(i)
        lo = start_of(bounds, pb * BLK) // CHUNK
        hi = pb // 2
        need[hi] = 1

        def add(ch, g, i=i):
            step_i[g] = i
            step_ch[g] = ch
            need[ch] = 1
            return g + 1

        count = lax.fori_loop(lo, hi, add, count)
    step_i[count] = 3
    step_ch[count] = block_of(3) // 2

    for cp in first:
        cp.wait()
    for j in range(8):
        t = lax.rem(m["z"] + RING[j] + 8, 8)
        row = pl.multiple_of(feature_row(m, t, 192), 64)
        for n in range(6):
            w[pl.ds(row, 192), n * 128 : (n + 1) * 128] = wp[j, n * 6 : n * 6 + 6].reshape(192, 128)
        row = pl.multiple_of(feature_row(m, t, 64), 64)
        for n in range(8):
            kvw[pl.ds(row, 64), n * 128 : (n + 1) * 128] = wp[j, 36 + n * 2 : 38 + n * 2].reshape(64, 128)

    lane = lax.broadcasted_iota(jnp.int32, (BLK, 128), 1)
    line = lax.broadcasted_iota(jnp.int32, (BLK, 128), 0)
    for half in range(2):
        full = jnp.dot(q[half], w[...], preferred_element_type=f32)
        for b in range(2):
            part = slice(b * BLK, (b + 1) * BLK)
            rows = slice(half * 256 + b * BLK, half * 256 + (b + 1) * BLK)
            label = label_of(bounds, line + block_of(half * 2 + b) * BLK)
            onehot = jnp.where(lane == label + 64, 1.0, 0.0)
            cos, sin = cs[rows, :128], cs[rows, 128:]
            x, y = full[part, 512:640], full[part, 640:]
            rot = (x * cos - y * sin, y * cos + x * sin)
            for h in range(4):
                r0 = pltpu.roll(rot[0], (128 - 32 * h) % 128, 1) if h else rot[0]
                r1 = pltpu.roll(rot[1], (32 - 32 * h) % 128, 1) if h != 1 else rot[1]
                tail = jnp.where(lane < 32, r0, jnp.where(lane < 64, r1, onehot))
                qs[h, rows, :128] = full[part, h * 128 : (h + 1) * 128].astype(bf16)
                qs[h, rows, 128:] = tail.astype(bf16)

    mx[...] = jnp.full(mx.shape, masked_value, f32)
    acc[...] = jnp.zeros(acc.shape, f32)
    total[...] = jnp.zeros(total.shape, f32)
    sbuf[EMPTY] = jnp.full((4, BLK, CHUNK), masked_value, f32)
    for cp in second:
        cp.wait()

    def place(i):
        zz = lax.rem(m["z"] + ring_shift(lax.rem(i, 8)) + 8, 8)
        return (zz * 2 + jnp.where(i < 8, m["c"], 1 - m["c"])) * 2

    def pick(i, n):
        base = place(i)
        use[n] = i
        return n + jnp.minimum(need[order[0, base] // 2] + need[order[0, base + 1] // 2], 1)

    used = lax.fori_loop(0, 16, pick, jnp.int32(0))

    def project(n, carry):
        for i in (use[2 * n], use[jnp.minimum(2 * n + 1, used - 1)]):
            base = place(i)
            x = jnp.concatenate([lat[e, i].reshape(256, 128) for e in range(4)], axis=1)
            y = jnp.dot(x, kvw[...], preferred_element_type=f32)
            fold = rope[i]
            for b in range(2):
                pb = pl.multiple_of(order[0, base + b] * BLK, BLK)
                rows = slice(b * BLK, (b + 1) * BLK)
                kn[pl.ds(pb, BLK), :] = y[rows, :512].astype(bf16)
                v[pl.ds(pb, BLK), :] = y[rows, 512:].astype(bf16)
                label = label_of(bounds, line[:, :64] + pb)
                apart = jnp.where((lane[:, :64] < 4) & (lane[:, :64] != label), masked_value, 0.0)
                kr[pl.ds(pb, BLK), :] = jnp.concatenate(
                    [fold[:, b * 64 : b * 64 + 64], apart.astype(bf16)], axis=1
                )
        return carry

    lax.fori_loop(0, (used + 1) // 2, project, 0)

    def scores(i, ch):
        keys = pl.ds(pl.multiple_of(ch * CHUNK, CHUNK), CHUNK)
        rows = pl.ds(pl.multiple_of(i * BLK, BLK), BLK)
        got = []
        for h in range(4):
            k = jnp.concatenate([kn[keys, h * 128 : (h + 1) * 128], kr[keys, :]], axis=1)
            got.append(
                lax.dot_general(
                    qs[h, rows, :], k, (((1,), (1,)), ((), ())), preferred_element_type=f32
                )
            )
        return got

    def keep(i, slot, h, s):
        sbuf[slot, h] = s
        mx[i, h] = jnp.maximum(mx[i, h], jnp.maximum(s[:, :128], s[:, 128:]))

    def diagonal(i, carry):
        pb = block_of(i)
        ch = pb // 2
        row = lax.broadcasted_iota(jnp.int32, (BLK, CHUNK), 0) + (pb * BLK - ch * CHUNK)
        col = lax.broadcasted_iota(jnp.int32, (BLK, CHUNK), 1)
        bias = jnp.where(col <= row, 0.0, masked_value)
        for h, s in enumerate(scores(i, ch)):
            keep(i, i, h, s + bias)
        return carry

    lax.fori_loop(0, 4, diagonal, 0)

    def score_four(n, carry):
        picks = []
        for e in range(4):
            g = jnp.minimum(4 * n + e, count - 1)
            i, ch = step_i[g], step_ch[g]
            picks.append((i, g + 4, scores(i, ch)))
        for i, slot, got in picks:
            for h, s in enumerate(got):
                keep(i, slot, h, s)
        return carry

    fours = (count + 3) // 4
    lax.fori_loop(0, fours, score_four, 0)

    hm[...] = jnp.full(hm.shape, masked_value, f32)

    def finish_max(i, carry):
        for h in range(4):
            top = jnp.broadcast_to(jnp.max(mx[i, h], axis=1, keepdims=True), (BLK, 128))
            rm[i, h] = top * to_exp2
            best = jnp.max(top, axis=0, keepdims=True) * scale
            best = jnp.where(lane[:1] == m["c"] * 4 + h, best, masked_value)
            hm[:1, :] = jnp.maximum(hm[:1, :], best)
        return carry

    lax.fori_loop(0, 4, finish_max, 0)
    hm_out[...] = jnp.broadcast_to(hm[:1, :8].reshape(1, 1, 8), (32, 1, 8))

    def mix(steps):
        for i, ch, slot in steps:
            keys = pl.ds(pl.multiple_of(ch * CHUNK, CHUNK), CHUNK)
            for h in range(4):
                s = sbuf[slot, h]
                top = rm[i, h]
                p0 = jnp.exp2(s[:, :128] * to_exp2 - top)
                p1 = jnp.exp2(s[:, 128:] * to_exp2 - top)
                total[i, h] += p0 + p1
                p = jnp.concatenate([p0, p1], axis=1).astype(bf16)
                acc[i, h] += jnp.dot(p, v[keys, h * 128 : (h + 1) * 128], preferred_element_type=f32)

    def mix_diagonal(n, carry):
        mix([(2 * n + e, block_of(2 * n + e) // 2, 2 * n + e) for e in range(2)])
        return carry

    lax.fori_loop(0, 2, mix_diagonal, 0)

    def mix_four(n, carry):
        steps = []
        for e in range(4):
            g = 4 * n + e
            at = jnp.minimum(g, count)
            steps.append((step_i[at], step_ch[at], jnp.where(g < count, g + 4, EMPTY)))
        mix(steps)
        return carry

    lax.fori_loop(0, fours, mix_four, 0)

    for to, first_block in ((out, 0), (out_send, 2)):

        def finish(i, carry, to=to, first_block=first_block):
            rows = pl.ds(pl.multiple_of(i * BLK, BLK), BLK)
            for h in range(4):
                whole = jnp.sum(total[i + first_block, h], axis=1, keepdims=True)
                to[rows, h * 128 : (h + 1) * 128] = (acc[i + first_block, h] / whole).astype(bf16)
            return carry

        lax.fori_loop(0, 2, finish, 0)


def shift_seq(by):
    return [(i, (i + 2 * by) % 16) for i in range(16)]


SWAP = [(i, i ^ 1) for i in range(16)]
XSWAP = [(i, i ^ 4) for i in range(8)]


def shift_y(by):
    return [(x * 4 + y, x * 4 + (y + by) % 4) for x in range(2) for y in range(4)]


def move(x, axis, perm):
    return lax.ppermute(x, axis, perm)


def ring(x, last=4):
    up, dn, got = x, x, [x]
    for s in range(1, last + 1):
        up = move(up, "seq", shift_seq(1))
        got.append(up)
        if s < 4:
            dn = move(dn, "seq", shift_seq(-1))
            got.append(dn)
    return got


def swap(x):
    return move(x, "seq", SWAP)


def call(kernel, outs, args, specs=None, scratch=()):
    outs = [jax.ShapeDtypeStruct(shape, dtype) for shape, dtype in outs]
    size = sum(math.prod(o.shape) * o.dtype.itemsize for o in outs)
    return pl.pallas_call(
        kernel,
        out_shape=outs,
        in_specs=specs or [VMEM] * len(args),
        out_specs=[VMEM] * len(outs),
        scratch_shapes=list(scratch),
        cost_estimate=pl.CostEstimate(flops=1 << 20, bytes_accessed=2 * size, transcendentals=0),
    )(*args)


def on_device(query_latent, key_latent, rope_key, w_uq, w_uk, w_uv, block_order, segment_ids):
    bf16, f32 = jnp.bfloat16, jnp.float32
    c = where_am_i()["c"]
    k_t, q_t = key_latent[0].T, query_latent[0].T
    k_tx, q_tx = move(k_t, "tp", XSWAP), move(q_t, "tp", XSWAP)
    w_mine, w_send, kv_mine, kv_send = call(
        split_kernel, [((18, 32, 128), bf16)] * 2 + [((8, 32, 128), bf16)] * 2, (w_uq, w_uk, w_uv)
    )
    w_other = swap(w_send)
    kv_other = swap(kv_send)
    cs, share = call(
        turn_kernel,
        [((512, 256), f32), ((32, 128), bf16)],
        (block_order, rope_key[0].T),
        specs=[SMEM, VMEM],
        scratch=[pltpu.VMEM((128, 128), bf16)],
    )
    k_one, w_one, q_x = call(
        pack_kernel,
        [((9, 32, 128), bf16), ((52, 32, 128), bf16), ((256, 384), bf16)],
        (k_t, k_tx, q_t, q_tx, share, w_mine, w_other, kv_mine, kv_other),
    )

    k_ring = ring(k_one)
    w_ring = ring(w_one, 3)
    w_ring += [move(w_ring[5][:26], "seq", shift_seq(1)), move(w_ring[6][26:], "seq", shift_seq(-1))]
    q_parts = [q_x] + [move(q_x, "tp", shift_y(by)) for by in (1, -1, 2)]
    q_own = jnp.concatenate(q_parts, axis=1)
    q_sib = swap(q_own)
    (k_all,) = call(
        join_kernel,
        [((8, 9, 32, 128), bf16)],
        k_ring,
        specs=[ANY] * 8,
        scratch=[pltpu.SemaphoreType.DMA((8,))],
    )
    k_up = move(k_all, "tp", shift_y(1))
    k_dn = move(k_all, "tp", shift_y(-1))
    k_f1 = move(k_up[:4], "tp", shift_y(1))
    k_f2 = move(k_dn[4:], "tp", shift_y(-1))
    k_own = [k_all, k_up, k_dn, k_f1, k_f2]
    k_sib = [swap(p) for p in k_own]

    vm = pltpu.VMEM
    ctx, ctx_send, everyone = pl.pallas_call(
        attend_kernel,
        out_shape=[
            jax.ShapeDtypeStruct((256, 512), bf16),
            jax.ShapeDtypeStruct((256, 512), bf16),
            jax.ShapeDtypeStruct((32, 1, 8), f32),
        ],
        in_specs=[SMEM, VMEM] + [ANY] * 11 + [VMEM] + [ANY] * 10,
        out_specs=[VMEM] * 3,
        scratch_shapes=[
            vm((8, 128), f32),
            vm((2, 256, 1536), bf16),
            vm((8, 52, 32, 128), bf16),
            vm((1536, 768), bf16),
            vm((512, 1024), bf16),
            vm((4, 16, 8, 32, 128), bf16),
            vm((16, 128, 128), bf16),
            vm((4096, 512), bf16),
            vm((4096, 512), bf16),
            vm((4096, 128), bf16),
            vm((4, 512, 256), bf16),
            vm((SLOTS, 4, BLK, CHUNK), f32),
            vm((4, 4, BLK, 128), f32),
            vm((4, 4, BLK, 128), f32),
            vm((4, 4, BLK, 128), f32),
            vm((4, 4, BLK, 128), f32),
            pltpu.SMEM((40,), jnp.int32),
            pltpu.SMEM((40,), jnp.int32),
            pltpu.SMEM((16,), jnp.int32),
            pltpu.SMEM((17,), jnp.int32),
            pltpu.SemaphoreType.DMA((2,)),
            pltpu.SemaphoreType.DMA((9,)),
            pltpu.SemaphoreType.DMA((2, 5, 2)),
        ],
        compiler_params=pltpu.CompilerParams(vmem_limit_bytes=60 << 20),
        cost_estimate=pl.CostEstimate(
            flops=20 << 30, bytes_accessed=12 << 20, transcendentals=4 << 20
        ),
        name="attend",
    )(block_order, segment_ids[0].reshape(32, 128), q_own, q_sib, *w_ring, cs, *k_own, *k_sib)

    everyone = lax.all_to_all(everyone, ("seq", "dp"), split_axis=0, concat_axis=0, tiled=True)
    got = swap(ctx_send)
    first = c == 0
    context = jnp.concatenate([jnp.where(first, ctx, got), jnp.where(first, got, ctx)], axis=1)
    everyone, context = lax.optimization_barrier((everyone, context))
    clipped_uq, clipped_uk = call(
        clip_kernel, [((96, 1536), bf16), ((32, 1024), bf16)], (everyone, w_uq, w_uk)
    )
    return (context[None], clipped_uq, clipped_uk)


def solution(mesh):
    placed = (
        P("dp", "seq", "tp"),
        P("dp", "seq", "tp"),
        P("dp", "seq", None),
        P("seq", "tp"),
        P("seq", "tp"),
        P("seq", "tp"),
        P("dp", None),
        P("dp", None),
    )
    return jax.shard_map(
        on_device,
        mesh=mesh,
        in_specs=placed,
        out_specs=(P("dp", "seq", "tp"), P("seq", "tp"), P("seq", "tp")),
        check_vma=False,
    )
```

```python
import math

import jax
import jax.numpy as jnp
from jax import lax
from jax.experimental import pallas as pl
from jax.experimental.pallas import tpu as pltpu
from jax.sharding import PartitionSpec as P


NOPE = 128
ROPE = 64
CLIP = 8
BLK = 128
CHUNK = 256

rope_base = 50000.0
masked_value = -1e30
scale = 1.0 / math.sqrt(NOPE + ROPE)

ANY = pl.BlockSpec(memory_space=pl.ANY)
SMEM = pl.BlockSpec(memory_space=pltpu.SMEM)
VMEM = pl.BlockSpec(memory_space=pltpu.VMEM)


def where_am_i():
    s, t = lax.axis_index("seq"), lax.axis_index("tp")
    return dict(z=s // 2, c=lax.rem(s, 2), y=lax.rem(t, 4), xl=t // 4)


def start_of(bounds, p):
    s = jnp.int32(0)
    for b in bounds:
        s = jnp.where(b <= p, jnp.maximum(s, b), s)
    return s


def feature_row(m, t, each):
    x, yy = t // 4, t % 4
    dy = lax.rem(yy - m["y"] + 4, 4)
    j = jnp.where(dy == 0, 0, jnp.where(dy == 1, 2, jnp.where(dy == 2, 3, 1)))
    xr = jnp.where(x == m["xl"], 0, 1)
    return (j * 2 + xr) * each


RING = [0, -1, 1, -2, 2, -3, 3, -4]


def ring_shift(j):
    return jnp.where(lax.rem(j, 2) == 1, -((j + 1) // 2), (j + 1) // 2)


W_COLS = [[h * 192 + e * 32 for e in range(4)] for h in range(4)] + [
    [h * 192 + 128 for h in range(4)],
    [h * 192 + 160 for h in range(4)],
]


def split_kernel(w_uq, w_uk, w_uv, w_mine, w_send, kv_mine, kv_send):
    c = where_am_i()["c"]

    def halves(own):
        for to, half in ((w_mine, own), (w_send, 1 - own)):
            for n, cols in enumerate(W_COLS):
                base = half * 768
                if n < 4:
                    block = w_uq[:, base + cols[0] : base + cols[0] + 128]
                else:
                    block = jnp.concatenate([w_uq[:, base + k : base + k + 32] for k in cols], axis=1)
                for b in range(3):
                    to[n * 3 + b] = block[b * 32 : (b + 1) * 32]
        for to, half in ((kv_mine, own), (kv_send, 1 - own)):
            for n in range(4):
                cols = slice(half * 512 + n * 128, half * 512 + n * 128 + 128)
                to[n] = w_uk[:, cols]
                to[4 + n] = w_uv[:, cols]

    @pl.when(c == 0)
    def _():
        halves(0)

    @pl.when(c == 1)
    def _():
        halves(1)


def turn_kernel(order, rope_t, cs, share, fold):
    m = where_am_i()
    pos = []
    lane = lax.broadcasted_iota(jnp.int32, (32, BLK), 1)
    for i in range(4):
        core = m["c"] if i < 2 else 1 - m["c"]
        pos.append(lane + order[0, (m["z"] * 2 + core) * 2 + i % 2] * BLK)
    steps = lax.broadcasted_iota(jnp.int32, (32, 512), 0).astype(jnp.float32) * (2.0 / ROPE)
    freqs = jnp.exp(-math.log(rope_base) * steps)
    angle = jnp.concatenate(pos, axis=1).astype(jnp.float32) * freqs
    cos, sin = jnp.cos(angle), jnp.sin(angle)
    cs[...] = jnp.concatenate([cos] * 4 + [sin] * 4, axis=0).T
    r = rope_t[...].astype(jnp.float32)
    a, b, rc, rs = r[:32], r[32:], cos[:, :256], sin[:, :256]
    both = jnp.concatenate([a * rc - b * rs, b * rc + a * rs], axis=0)
    fold[...] = jnp.concatenate([both[:, :128], both[:, 128:]], axis=0).T.astype(jnp.bfloat16)
    share[...] = fold[pl.ds(pl.multiple_of(m["y"] * 32, 32), 32), :]


def pack_w_kernel(w_mine, w_other, kv_mine, kv_other, w_one):
    c = where_am_i()["c"]
    for core, w, kv in ((c, w_mine, kv_mine), (1 - c, w_other, kv_other)):
        for n in range(6):
            w_one[pl.ds(n * 6 + core * 3, 3)] = w[n * 3 : n * 3 + 3]
        for n in range(8):
            w_one[36 + n * 2 + core] = kv[n]


def pack_kernel(k_t, k_tx, q_t, q_tx, share, k_one, q_x):
    lat = jnp.concatenate([k_t[...], k_tx[...]], axis=0).T
    for b in range(8):
        k_one[b] = lat[b * 32 : (b + 1) * 32]
    k_one[8] = share[...]
    q_x[...] = jnp.concatenate([q_t[...], q_tx[...]], axis=0).T


def join_kernel(*refs):
    ins, out, sem = refs[:8], refs[8], refs[9]
    copies = [pltpu.make_async_copy(r, out.at[j], sem.at[j]) for j, r in enumerate(ins)]
    for cp in copies:
        cp.start()
    for cp in copies:
        cp.wait()


def clip_kernel(everyone, w_uq, w_uk, clipped_uq, clipped_uk):
    head_max = everyone[0]
    for n in range(1, 32):
        head_max = jnp.maximum(head_max, everyone[n])
    ratio = CLIP / jnp.maximum(head_max, CLIP)
    root = jnp.sqrt(ratio)
    for out, w, width in ((clipped_uq, w_uq, NOPE + ROPE), (clipped_uk, w_uk, NOPE)):
        lane = lax.broadcasted_iota(jnp.int32, (1, 8 * width), 1)
        factor = jnp.ones((1, 8 * width), jnp.float32)
        for h in range(8):
            here = jnp.where(lane < h * width + NOPE, root[:, h : h + 1], ratio[:, h : h + 1])
            factor = jnp.where(lane >= h * width, here, factor)
        out[...] = (w[...].astype(jnp.float32) * factor).astype(jnp.bfloat16)


def label_of(bounds, p):
    label = jnp.zeros_like(p)
    for b in bounds:
        label = label + jnp.where(p >= b, 1, 0)
    return label


SLOTS = 38
EMPTY = 37
to_exp2 = scale * math.log2(math.e)


def attend_kernel(order, seg, *refs):
    q_in, w_in, refs = refs[:2], refs[2:11], refs[1:]
    cs, pieces = refs[10], (refs[11:16], refs[16:21])
    out, out_send, hm_out = refs[21:24]
    hm, q, wp, w, kvw, lat, rope, kn, v, kr, qs, sbuf, mx, rm, acc, total, step_i, step_ch, need, use = refs[24:44]
    qsem, wsem, ksem = refs[44:]
    m = where_am_i()

    def block_of(i):
        core = jnp.where(i // 2 == 0, m["c"], 1 - m["c"])
        return order[0, (m["z"] * 2 + core) * 2 + lax.rem(i, 2)]

    f32, bf16 = jnp.float32, jnp.bfloat16
    first, second = [], []
    for half in range(2):
        first.append(pltpu.make_async_copy(q_in[half], q.at[half], qsem.at[half]))
    for j in range(7):
        first.append(pltpu.make_async_copy(w_in[j], wp.at[j], wsem.at[j]))
    for e in range(2):
        first.append(pltpu.make_async_copy(w_in[7 + e], wp.at[7, pl.ds(26 * e, 26)], wsem.at[7 + e]))
    for core in range(2):
        own, up, dn, f1, f2 = pieces[core]
        for n, (src, plane, start, count, dy) in enumerate(
            ((own, 0, 0, 8, 0), (up, 1, 0, 8, 3), (dn, 2, 0, 8, 1), (f1, 3, 0, 4, 2), (f2, 3, 4, 4, 2))
        ):
            rows = pl.ds(core * 8 + start, count)
            yq = pl.multiple_of(lax.rem(m["y"] + dy, 4) * 32, 32)
            second.append(
                pltpu.make_async_copy(src.at[:, :8], lat.at[plane, rows], ksem.at[core, n, 0])
            )
            second.append(
                pltpu.make_async_copy(
                    src.at[:, 8], rope.at[rows, pl.ds(yq, 32), :], ksem.at[core, n, 1]
                )
            )
    for cp in first + second:
        cp.start()

    bounds = [jnp.sum(jnp.where(seg[...] < l, 1, 0)) for l in (1, 2, 3)]

    for n in range(16):
        need[n] = 0
    count = jnp.int32(0)
    for i in range(4):
        pb = block_of(i)
        lo = start_of(bounds, pb * BLK) // CHUNK
        hi = pb // 2
        need[hi] = 1

        def add(ch, g, i=i):
            step_i[g] = i
            step_ch[g] = ch
            need[ch] = 1
            return g + 1

        count = lax.fori_loop(lo, hi, add, count)
    step_i[count] = 3
    step_ch[count] = block_of(3) // 2

    for cp in first:
        cp.wait()
    for j in range(8):
        t = lax.rem(m["z"] + RING[j] + 8, 8)
        row = pl.multiple_of(feature_row(m, t, 192), 64)
        for n in range(6):
            w[pl.ds(row, 192), n * 128 : (n + 1) * 128] = wp[j, n * 6 : n * 6 + 6].reshape(192, 128)
        row = pl.multiple_of(feature_row(m, t, 64), 64)
        for n in range(8):
            kvw[pl.ds(row, 64), n * 128 : (n + 1) * 128] = wp[j, 36 + n * 2 : 38 + n * 2].reshape(64, 128)

    lane = lax.broadcasted_iota(jnp.int32, (BLK, 128), 1)
    line = lax.broadcasted_iota(jnp.int32, (BLK, 128), 0)
    for half in range(2):
        full = jnp.dot(q[half], w[...], preferred_element_type=f32)
        for b in range(2):
            part = slice(b * BLK, (b + 1) * BLK)
            rows = slice(half * 256 + b * BLK, half * 256 + (b + 1) * BLK)
            label = label_of(bounds, line + block_of(half * 2 + b) * BLK)
            onehot = jnp.where(lane == label + 64, 1.0, 0.0)
            cos, sin = cs[rows, :128], cs[rows, 128:]
            x, y = full[part, 512:640], full[part, 640:]
            rot = (x * cos - y * sin, y * cos + x * sin)
            for h in range(4):
                r0 = pltpu.roll(rot[0], (128 - 32 * h) % 128, 1) if h else rot[0]
                r1 = pltpu.roll(rot[1], (32 - 32 * h) % 128, 1) if h != 1 else rot[1]
                tail = jnp.where(lane < 32, r0, jnp.where(lane < 64, r1, onehot))
                qs[h, rows, :128] = full[part, h * 128 : (h + 1) * 128].astype(bf16)
                qs[h, rows, 128:] = tail.astype(bf16)

    mx[...] = jnp.full(mx.shape, masked_value, f32)
    acc[...] = jnp.zeros(acc.shape, f32)
    total[...] = jnp.zeros(total.shape, f32)
    sbuf[EMPTY] = jnp.full((4, BLK, CHUNK), masked_value, f32)
    for cp in second:
        cp.wait()

    def place(i):
        zz = lax.rem(m["z"] + ring_shift(lax.rem(i, 8)) + 8, 8)
        return (zz * 2 + jnp.where(i < 8, m["c"], 1 - m["c"])) * 2

    def pick(i, n):
        base = place(i)
        use[n] = i
        return n + jnp.minimum(need[order[0, base] // 2] + need[order[0, base + 1] // 2], 1)

    used = lax.fori_loop(0, 16, pick, jnp.int32(0))

    def project(n, carry):
        for i in (use[2 * n], use[jnp.minimum(2 * n + 1, used - 1)]):
            base = place(i)
            x = jnp.concatenate([lat[e, i].reshape(256, 128) for e in range(4)], axis=1)
            y = jnp.dot(x, kvw[...], preferred_element_type=f32)
            fold = rope[i]
            for b in range(2):
                pb = pl.multiple_of(order[0, base + b] * BLK, BLK)
                rows = slice(b * BLK, (b + 1) * BLK)
                kn[pl.ds(pb, BLK), :] = y[rows, :512].astype(bf16)
                v[pl.ds(pb, BLK), :] = y[rows, 512:].astype(bf16)
                label = label_of(bounds, line[:, :64] + pb)
                apart = jnp.where((lane[:, :64] < 4) & (lane[:, :64] != label), masked_value, 0.0)
                kr[pl.ds(pb, BLK), :] = jnp.concatenate(
                    [fold[:, b * 64 : b * 64 + 64], apart.astype(bf16)], axis=1
                )
        return carry

    lax.fori_loop(0, (used + 1) // 2, project, 0)

    def scores(i, ch):
        keys = pl.ds(pl.multiple_of(ch * CHUNK, CHUNK), CHUNK)
        rows = pl.ds(pl.multiple_of(i * BLK, BLK), BLK)
        got = []
        for h in range(4):
            k = jnp.concatenate([kn[keys, h * 128 : (h + 1) * 128], kr[keys, :]], axis=1)
            got.append(
                lax.dot_general(
                    qs[h, rows, :], k, (((1,), (1,)), ((), ())), preferred_element_type=f32
                )
            )
        return got

    def keep(i, slot, h, s):
        sbuf[slot, h] = s
        mx[i, h] = jnp.maximum(mx[i, h], jnp.maximum(s[:, :128], s[:, 128:]))

    def diagonal(i, carry):
        pb = block_of(i)
        ch = pb // 2
        row = lax.broadcasted_iota(jnp.int32, (BLK, CHUNK), 0) + (pb * BLK - ch * CHUNK)
        col = lax.broadcasted_iota(jnp.int32, (BLK, CHUNK), 1)
        bias = jnp.where(col <= row, 0.0, masked_value)
        for h, s in enumerate(scores(i, ch)):
            keep(i, i, h, s + bias)
        return carry

    lax.fori_loop(0, 4, diagonal, 0)

    def score_four(n, carry):
        picks = []
        for e in range(4):
            g = jnp.minimum(4 * n + e, count - 1)
            i, ch = step_i[g], step_ch[g]
            picks.append((i, g + 4, scores(i, ch)))
        for i, slot, got in picks:
            for h, s in enumerate(got):
                keep(i, slot, h, s)
        return carry

    fours = (count + 3) // 4
    lax.fori_loop(0, fours, score_four, 0)

    hm[...] = jnp.full(hm.shape, masked_value, f32)

    def finish_max(i, carry):
        for h in range(4):
            top = jnp.broadcast_to(jnp.max(mx[i, h], axis=1, keepdims=True), (BLK, 128))
            rm[i, h] = top * to_exp2
            best = jnp.max(top, axis=0, keepdims=True) * scale
            best = jnp.where(lane[:1] == m["c"] * 4 + h, best, masked_value)
            hm[:1, :] = jnp.maximum(hm[:1, :], best)
        return carry

    lax.fori_loop(0, 4, finish_max, 0)
    hm_out[...] = jnp.broadcast_to(hm[:1, :8].reshape(1, 1, 8), (32, 1, 8))

    def mix(steps):
        for i, ch, slot in steps:
            keys = pl.ds(pl.multiple_of(ch * CHUNK, CHUNK), CHUNK)
            for h in range(4):
                s = sbuf[slot, h]
                top = rm[i, h]
                p0 = jnp.exp2(s[:, :128] * to_exp2 - top)
                p1 = jnp.exp2(s[:, 128:] * to_exp2 - top)
                total[i, h] += p0 + p1
                p = jnp.concatenate([p0, p1], axis=1).astype(bf16)
                acc[i, h] += jnp.dot(p, v[keys, h * 128 : (h + 1) * 128], preferred_element_type=f32)

    def mix_diagonal(n, carry):
        mix([(2 * n + e, block_of(2 * n + e) // 2, 2 * n + e) for e in range(2)])
        return carry

    lax.fori_loop(0, 2, mix_diagonal, 0)

    def mix_four(n, carry):
        steps = []
        for e in range(4):
            g = 4 * n + e
            at = jnp.minimum(g, count)
            steps.append((step_i[at], step_ch[at], jnp.where(g < count, g + 4, EMPTY)))
        mix(steps)
        return carry

    lax.fori_loop(0, fours, mix_four, 0)

    for to, first_block in ((out, 0), (out_send, 2)):

        def finish(i, carry, to=to, first_block=first_block):
            rows = pl.ds(pl.multiple_of(i * BLK, BLK), BLK)
            for h in range(4):
                whole = jnp.sum(total[i + first_block, h], axis=1, keepdims=True)
                to[rows, h * 128 : (h + 1) * 128] = (acc[i + first_block, h] / whole).astype(bf16)
            return carry

        lax.fori_loop(0, 2, finish, 0)


def shift_seq(by):
    return [(i, (i + 2 * by) % 16) for i in range(16)]


SWAP = [(i, i ^ 1) for i in range(16)]
XSWAP = [(i, i ^ 4) for i in range(8)]


def shift_y(by):
    return [(x * 4 + y, x * 4 + (y + by) % 4) for x in range(2) for y in range(4)]


def move(x, axis, perm):
    return lax.ppermute(x, axis, perm)


def ring(x, last=4):
    up, dn, got = x, x, [x]
    for s in range(1, last + 1):
        up = move(up, "seq", shift_seq(1))
        got.append(up)
        if s < 4:
            dn = move(dn, "seq", shift_seq(-1))
            got.append(dn)
    return got


def swap(x):
    return move(x, "seq", SWAP)


def call(kernel, outs, args, specs=None, scratch=()):
    outs = [jax.ShapeDtypeStruct(shape, dtype) for shape, dtype in outs]
    size = sum(math.prod(o.shape) * o.dtype.itemsize for o in outs)
    return pl.pallas_call(
        kernel,
        out_shape=outs,
        in_specs=specs or [VMEM] * len(args),
        out_specs=[VMEM] * len(outs),
        scratch_shapes=list(scratch),
        cost_estimate=pl.CostEstimate(flops=1 << 20, bytes_accessed=2 * size, transcendentals=0),
    )(*args)


def on_device(query_latent, key_latent, rope_key, w_uq, w_uk, w_uv, block_order, segment_ids):
    bf16, f32 = jnp.bfloat16, jnp.float32
    c = where_am_i()["c"]
    k_t, q_t = key_latent[0].T, query_latent[0].T
    k_tx, q_tx = move(k_t, "tp", XSWAP), move(q_t, "tp", XSWAP)
    w_mine, w_send, kv_mine, kv_send = call(
        split_kernel, [((18, 32, 128), bf16)] * 2 + [((8, 32, 128), bf16)] * 2, (w_uq, w_uk, w_uv)
    )
    w_other = swap(w_send)
    kv_other = swap(kv_send)
    cs, share = call(
        turn_kernel,
        [((512, 256), f32), ((32, 128), bf16)],
        (block_order, rope_key[0].T),
        specs=[SMEM, VMEM],
        scratch=[pltpu.VMEM((128, 128), bf16)],
    )
    k_one, q_x = call(
        pack_kernel, [((9, 32, 128), bf16), ((256, 384), bf16)], (k_t, k_tx, q_t, q_tx, share)
    )
    (w_one,) = call(pack_w_kernel, [((52, 32, 128), bf16)], (w_mine, w_other, kv_mine, kv_other))

    k_ring = ring(k_one)
    w_ring = ring(w_one, 3)
    w_ring += [move(w_ring[5][:26], "seq", shift_seq(1)), move(w_ring[6][26:], "seq", shift_seq(-1))]
    q_parts = [q_x] + [move(q_x, "tp", shift_y(by)) for by in (1, -1, 2)]
    q_own = jnp.concatenate(q_parts, axis=1)
    q_sib = swap(q_own)
    (k_all,) = call(
        join_kernel,
        [((8, 9, 32, 128), bf16)],
        k_ring,
        specs=[ANY] * 8,
        scratch=[pltpu.SemaphoreType.DMA((8,))],
    )
    k_up = move(k_all, "tp", shift_y(1))
    k_dn = move(k_all, "tp", shift_y(-1))
    k_f1 = move(k_up[:4], "tp", shift_y(1))
    k_f2 = move(k_dn[4:], "tp", shift_y(-1))
    k_own = [k_all, k_up, k_dn, k_f1, k_f2]
    k_sib = [swap(p) for p in k_own]

    vm = pltpu.VMEM
    ctx, ctx_send, everyone = pl.pallas_call(
        attend_kernel,
        out_shape=[
            jax.ShapeDtypeStruct((256, 512), bf16),
            jax.ShapeDtypeStruct((256, 512), bf16),
            jax.ShapeDtypeStruct((32, 1, 8), f32),
        ],
        in_specs=[SMEM, VMEM] + [ANY] * 11 + [VMEM] + [ANY] * 10,
        out_specs=[VMEM] * 3,
        scratch_shapes=[
            vm((8, 128), f32),
            vm((2, 256, 1536), bf16),
            vm((8, 52, 32, 128), bf16),
            vm((1536, 768), bf16),
            vm((512, 1024), bf16),
            vm((4, 16, 8, 32, 128), bf16),
            vm((16, 128, 128), bf16),
            vm((4096, 512), bf16),
            vm((4096, 512), bf16),
            vm((4096, 128), bf16),
            vm((4, 512, 256), bf16),
            vm((SLOTS, 4, BLK, CHUNK), f32),
            vm((4, 4, BLK, 128), f32),
            vm((4, 4, BLK, 128), f32),
            vm((4, 4, BLK, 128), f32),
            vm((4, 4, BLK, 128), f32),
            pltpu.SMEM((40,), jnp.int32),
            pltpu.SMEM((40,), jnp.int32),
            pltpu.SMEM((16,), jnp.int32),
            pltpu.SMEM((17,), jnp.int32),
            pltpu.SemaphoreType.DMA((2,)),
            pltpu.SemaphoreType.DMA((9,)),
            pltpu.SemaphoreType.DMA((2, 5, 2)),
        ],
        compiler_params=pltpu.CompilerParams(vmem_limit_bytes=60 << 20),
        cost_estimate=pl.CostEstimate(
            flops=20 << 30, bytes_accessed=12 << 20, transcendentals=4 << 20
        ),
        name="attend",
    )(block_order, segment_ids[0].reshape(32, 128), q_own, q_sib, *w_ring, cs, *k_own, *k_sib)

    everyone = lax.all_to_all(everyone, ("seq", "dp"), split_axis=0, concat_axis=0, tiled=True)
    got = swap(ctx_send)
    first = c == 0
    context = jnp.concatenate([jnp.where(first, ctx, got), jnp.where(first, got, ctx)], axis=1)
    everyone, context = lax.optimization_barrier((everyone, context))
    clipped_uq, clipped_uk = call(
        clip_kernel, [((96, 1536), bf16), ((32, 1024), bf16)], (everyone, w_uq, w_uk)
    )
    return (context[None], clipped_uq, clipped_uk)


def solution(mesh):
    placed = (
        P("dp", "seq", "tp"),
        P("dp", "seq", "tp"),
        P("dp", "seq", None),
        P("seq", "tp"),
        P("seq", "tp"),
        P("seq", "tp"),
        P("dp", None),
        P("dp", None),
    )
    return jax.shard_map(
        on_device,
        mesh=mesh,
        in_specs=placed,
        out_specs=(P("dp", "seq", "tp"), P("seq", "tp"), P("seq", "tp")),
        check_vma=False,
    )
```
